32 devices in a mesh: rows: 8 (over z, x), cols: 4 (over y, core).
Axes of the slice: x: 2, y: 2, z: 4, core: 2. Of those that a mesh axis runs over, the one named last changes fastest.
Arguments:
- tables: float32 [4, 4096, 512], P(None, 'rows', 'cols'), may hold values from -1.5 to 1.5
- dense_features: float32 [256, 512], P('rows', 'cols'), may hold values from -6 to 6
- slot_rows: int32 [8, 8, 4, 64], P('rows'), may hold values from 0 to 511, as said below
- slot_examples: int32 [8, 8, 4, 64], P('rows'), may hold values from 0 to 31, as said below
- slot_counts: int32 [8, 8, 4], P('rows'), may hold values from 21 to 64, as said below
Outputs:
- pooled: float32 [256, 4, 512], P('rows', None, 'cols')
- interactions: float32 [256, 10], P('rows')
The draws below stay inside these ranges and needn't reach their ends.
Inputs may be any that keep to these rules, and one draw needn't show every extreme that they name: slot_rows[s, o, t, c] names row o * 512 + value of table t. `slot_examples`: an example of the source device s. `slot_counts`: slots 0 to count - 1 of a bucket are live, the others unused; some bucket of every draw is full.
All inputs are finite; a program needn't handle non-finite values.
Results may differ from the reference program's by a relative error of at most 0.0003.
Values sent between devices are 32-bit elements; how exact they have to be, the bound alone decides.
A program may use at most 64 MiB of HBM per device.

```python
import jax
import jax.numpy as jnp
import numpy as np
from jax import lax

E = 512
TABLES = 4
ROWS_DEV = 512
B_DEV = 32
CAP = 64
BATCH = 256
TABLE_ROWS = 4096
N_ROWS = 8


def draw_slot_counts(key, part):
    first_key, second_key = jax.random.split(jax.random.fold_in(key, 11))
    base = jax.random.randint(first_key, (N_ROWS, N_ROWS, TABLES), CAP // 3, 2 * CAP // 3 + 1)
    hottest = jax.random.randint(second_key, (TABLES,), 0, N_ROWS)
    is_hot = jnp.arange(N_ROWS)[None, :, None] == hottest[None, None, :]
    return jnp.where(is_hot, CAP, base).astype(jnp.int32)


def draw_slot_rows(key, part):
    first_key, second_key, third_key = jax.random.split(jax.random.fold_in(key, 23), 3)
    shape_all = (N_ROWS, N_ROWS, TABLES, CAP)
    first_draw = jax.random.randint(first_key, shape_all, 0, ROWS_DEV)
    second_draw = jax.random.randint(second_key, shape_all, 0, ROWS_DEV)
    offsets = jax.random.randint(third_key, (N_ROWS, TABLES), 0, ROWS_DEV)
    skewed = first_draw * second_draw // ROWS_DEV
    return ((skewed + offsets[None, :, :, None]) % ROWS_DEV).astype(jnp.int32)


def draw_slot_examples(key, part):
    first_key, second_key = jax.random.split(jax.random.fold_in(key, 37))
    shape_all = (N_ROWS, N_ROWS, TABLES, CAP)
    first_draw = jax.random.randint(first_key, shape_all, 0, B_DEV)
    second_draw = jax.random.randint(second_key, shape_all, 0, B_DEV)
    return jnp.minimum(first_draw, second_draw).astype(jnp.int32)


def shard_levels(key, dims, cuts, least, top_value):
    def one(axis_at, blocks):
        heights = jax.random.uniform(jax.random.fold_in(jax.random.fold_in(key, 6), axis_at), (blocks,), jnp.float32, least / len(cuts), top_value / len(cuts))
        return jnp.repeat(jnp.exp(heights), dims[axis_at] // blocks).reshape((-1,) + (1,) * (len(dims) - axis_at - 1))

    factor_of = one(*cuts[0])
    for cut in cuts[1:]:
        factor_of = factor_of * one(*cut)
    return factor_of


def bell_draw(rng, extent, width, most, cuts=(), kind=jnp.bfloat16):
    array = jax.random.normal(rng, extent, jnp.float32) * width
    if len(cuts) > 0:
        array = shard_levels(rng, extent, cuts, -0.22, 0.18) * array
    return jnp.clip(array, min=-most, max=most).astype(kind)


def setup_inputs(seed: int = 0) -> dict:
    keys = jax.random.split(jax.random.key(seed), 6)
    tables = bell_draw(keys[0], (TABLES, TABLE_ROWS, E), 0.25, 1.5, ((1, 8), (2, 4)), jnp.float32)
    dense_features = bell_draw(keys[1], (BATCH, E), 1.0, 6.0, ((0, 8), (1, 4)), jnp.float32)
    slot_rows = draw_slot_rows(jax.random.fold_in(keys[5], 71), 0)
    slot_examples = draw_slot_examples(jax.random.fold_in(keys[5], 71), 0)
    slot_counts = draw_slot_counts(jax.random.fold_in(keys[5], 71), 0)
    return {"tables": tables, "dense_features": dense_features, "slot_rows": slot_rows, "slot_examples": slot_examples, "slot_counts": slot_counts}


def reference(tables, dense_features, slot_rows, slot_examples, slot_counts):
    slot_index = jnp.arange(CAP, dtype=jnp.int32)
    live_slots = slot_index[None, None, None, :] < slot_counts[:, :, :, None]
    owner_base = (jnp.arange(N_ROWS, dtype=jnp.int32) * ROWS_DEV)[:, None, None]
    table_index = jnp.arange(TABLES, dtype=jnp.int32)[None, :, None]

    def one_source(pieces):
        rows_here, examples_here, live_here = pieces
        global_rows = (rows_here + owner_base).astype(jnp.int32)
        looked = tables[table_index, global_rows]
        looked = jnp.where(live_here[:, :, :, None], looked, jnp.zeros_like(looked))
        segment_ids = (examples_here * TABLES + table_index).astype(jnp.int32)
        summed = jax.ops.segment_sum(looked.reshape(-1, E), segment_ids.reshape(-1), num_segments=B_DEV * TABLES)
        return summed.reshape(B_DEV, TABLES, E)

    pooled = lax.map(one_source, (slot_rows, slot_examples, live_slots)).reshape(BATCH, TABLES, E)
    vectors = jnp.concatenate([dense_features[:, None, :], pooled], axis=1)
    gram_matrix = jnp.einsum("bie,bje->bij", vectors, vectors, precision=lax.Precision.HIGHEST)
    pair_first, pair_second = np.triu_indices(TABLES + 1, 1)
    interactions = gram_matrix[:, pair_first, pair_second] * (E ** -0.5)
    return pooled, interactions
```

```python
import functools

import jax
import jax.numpy as jnp
from jax import lax
from jax.experimental import pallas as pl
from jax.experimental.pallas import tpu as pltpu
from jax.sharding import PartitionSpec as P

MESH = pl.DeviceIdType.MESH
CHUNKS = 2
DEAD = -65536


def kernel(
    n,
    cols,
    tables_hbm,
    dense_hbm,
    rows_hbm,
    examples_hbm,
    counts_hbm,
    pooled_ref,
    inter_ref,
    dense_ref,
    rows_ref,
    examples_ref,
    counts_ref,
    table_buf,
    split_buf,
    id_send,
    id_recv,
    pair_keep,
    pair_send,
    pair_recv,
    far_send,
    far_recv,
    near_recv,
    gram_recv,
    gram_send,
    load_sem,
    id_ssem,
    id_rsem,
    pair_ssem,
    pair_rsem,
    far_ssem,
    far_rsem,
    near_ssem,
    near_rsem,
    gram_ssem,
    gram_rsem,
):
    tables, range_rows, width = table_buf.shape
    here = dense_ref.shape[0]
    cap = rows_ref.shape[3]
    far = n // 2
    chunks = pair_ssem.shape[1]
    step = tables // chunks
    me = lax.axis_index("rows")
    col = lax.axis_index("cols")
    hi, lo = me // 2, me % 2
    mate = hi * 2 + (1 - lo)

    sources = (counts_hbm, rows_hbm, examples_hbm, tables_hbm, dense_hbm)
    targets = (counts_ref, rows_ref, examples_ref, table_buf, dense_ref)
    loads = [pltpu.make_async_copy(a, b, load_sem.at[i]) for i, (a, b) in enumerate(zip(sources, targets))]

    barrier = pltpu.get_barrier_semaphore()
    for j in range(1, n):
        pl.semaphore_signal(barrier, inc=1, device_id={"rows": (me + j) % n}, device_id_type=MESH)
    for j in range(1, cols):
        pl.semaphore_signal(barrier, inc=1, device_id={"cols": (col + j) % cols}, device_id_type=MESH)

    for load in loads:
        load.start()

    slot = lax.broadcasted_iota(jnp.int32, (tables, cap), 1)
    table_id = lax.broadcasted_iota(jnp.int32, (tables, cap), 0)
    for load in loads[:3]:
        load.wait()
    for p in range(n):
        count = jnp.full((tables, cap), counts_ref[0, 0, p], jnp.int32)
        for t in range(1, tables):
            count = jnp.where(table_id == t, counts_ref[0, t, p], count)
        rows_p = rows_ref[0, p]
        ex_p = jnp.where(slot < count, examples_ref[0, p], DEAD)
        id_send[p, 0:tables, :] = jnp.concatenate([rows_p, rows_p], axis=1)
        id_send[p, tables : 2 * tables, :] = jnp.concatenate([ex_p, ex_p], axis=1)

    pl.semaphore_wait(barrier, n - 1 + cols - 1)

    def group_of(k):
        return (hi // 2 + 1 + k // 2) % (far // 2) * 2 + (hi + 1 + k) % 2

    def id_copy(dst):
        return pltpu.make_async_remote_copy(
            src_ref=id_send.at[dst],
            dst_ref=id_recv.at[me],
            send_sem=id_ssem.at[dst],
            recv_sem=id_rsem.at[me],
            device_id={"rows": dst},
            device_id_type=MESH,
        )

    def id_wait(src):
        pltpu.make_async_remote_copy(
            src_ref=id_send.at[src],
            dst_ref=id_recv.at[src],
            send_sem=id_ssem.at[src],
            recv_sem=id_rsem.at[src],
            device_id={"rows": src},
            device_id_type=MESH,
        ).wait_recv()

    for k in range(far - 1):
        dst_hi = group_of(k)
        id_copy(dst_hi * 2 + lo).start()
        id_copy(dst_hi * 2 + (1 - lo)).start()
    id_copy(mate).start()
    id_recv[me] = id_send[me]

    loads[3].wait()
    for t in range(tables):
        whole = table_buf[t]
        high = whole.astype(jnp.bfloat16)
        split_buf[t, :, 0:width] = high
        split_buf[t, :, width : 2 * width] = (whole - high.astype(jnp.float32)).astype(jnp.bfloat16)

    first_half = lax.broadcasted_iota(jnp.int32, (tables, 2 * cap), 1) < cap
    offset = jnp.where(first_half, lo * here, (1 - lo) * here)
    row_iota = lax.broadcasted_iota(jnp.int32, (range_rows, 2 * cap), 0)
    ex_iota = lax.broadcasted_iota(jnp.int32, (2 * here, 2 * cap), 0)

    def pair_copy(g, c):
        piece = pl.ds(c * step, step)
        return pltpu.make_async_remote_copy(
            src_ref=pair_send.at[g, piece],
            dst_ref=pair_recv.at[g, piece],
            send_sem=pair_ssem.at[g, c],
            recv_sem=pair_rsem.at[g, c],
            device_id={"rows": mate},
            device_id_type=MESH,
        )

    def far_copy(g, c):
        piece = pl.ds(c * step, step)
        return pltpu.make_async_remote_copy(
            src_ref=far_send.at[g, piece],
            dst_ref=far_recv.at[hi, piece],
            send_sem=far_ssem.at[g, c],
            recv_sem=far_rsem.at[hi, c],
            device_id={"rows": g * 2 + lo},
            device_id_type=MESH,
        )

    def far_wait(g, c):
        piece = pl.ds(c * step, step)
        pltpu.make_async_remote_copy(
            src_ref=far_send.at[g, piece],
            dst_ref=far_recv.at[g, piece],
            send_sem=far_ssem.at[g, c],
            recv_sem=far_rsem.at[g, c],
            device_id={"rows": g * 2 + lo},
            device_id_type=MESH,
        ).wait_recv()

    near = hi + 1 - 2 * (hi % 2)

    def near_copy(same):
        return pltpu.make_async_remote_copy(
            src_ref=pair_keep.at[near] if same else pair_send.at[near],
            dst_ref=near_recv.at[0 if same else 1],
            send_sem=near_ssem.at[0 if same else 1],
            recv_sem=near_rsem.at[0 if same else 1],
            device_id={"rows": near * 2 + (lo if same else 1 - lo)},
            device_id_type=MESH,
        )

    def compute(g, paired=True):
        even = id_recv[g * 2]
        odd = id_recv[g * 2 + 1]
        row_of = jnp.where(first_half, even[0:tables], odd[0:tables])
        code = jnp.where(first_half, even[tables : 2 * tables], odd[tables : 2 * tables]) + offset
        for t in range(tables):
            row_hot = jnp.where(row_iota == row_of[t : t + 1], 1.0, 0.0).astype(jnp.bfloat16)
            ex_hot = jnp.where(ex_iota == code[t : t + 1], 1.0, 0.0).astype(jnp.bfloat16)
            hits = lax.dot_general(
                ex_hot, row_hot, (((1,), (1,)), ((), ())), preferred_element_type=jnp.float32
            ).astype(jnp.bfloat16)
            both = jnp.dot(hits, split_buf[t], preferred_element_type=jnp.float32)
            part = both[:, 0:width] + both[:, width : 2 * width]
            pair_keep[g, t] = part[0:here]
            pair_send[g, t] = part[here : 2 * here]
            if paired and (t + 1) % step == 0:
                pair_copy(g, t // step).start()

    def forward(g):
        for c in range(chunks):
            pair_copy(g, c).wait_recv()
            piece = pl.ds(c * step, step)
            far_send[g, piece] = pair_keep[g, piece] + pair_recv[g, piece]
            far_copy(g, c).start()

    def remote_group(g):
        id_wait(g * 2)
        id_wait(g * 2 + 1)
        compute(g)

    remote_group(group_of(0))
    if far <= 8:
        for k in range(1, far - 2):
            remote_group(group_of(k))
            forward(group_of(k - 1))
    else:

        @pl.loop(1, far - 2)
        def _(k):
            remote_group(group_of(k))
            forward(group_of(k - 1))

    id_wait(near * 2)
    id_wait(near * 2 + 1)
    compute(near, False)
    near_copy(True).start()
    near_copy(False).start()
    forward(group_of(far - 3))
    id_wait(mate)
    compute(hi)

    for c in range(chunks):
        pair_copy(hi, c).wait_recv()
    total = pair_keep[hi] + pair_recv[hi]
    for same in (True, False):
        near_copy(same).wait_recv()
    total = total + (near_recv[0] + near_recv[1])
    for k in range(far - 2):
        g = group_of(far - 3 - k)
        for c in range(chunks):
            far_wait(g, c)
        total = total + far_recv[g]

    for t in range(tables):
        pooled_ref[:, t, :] = total[t]
    loads[4].wait()
    vectors = [dense_ref[...]] + [total[t] for t in range(tables)]
    lane = lax.broadcasted_iota(jnp.int32, (here, 128), 1)
    gram = jnp.zeros((here, 128), jnp.float32)
    pair = 0
    for i in range(tables + 1):
        for j in range(i + 1, tables + 1):
            inner = jnp.sum(vectors[i] * vectors[j], axis=1, keepdims=True)
            gram = jnp.where(lane == pair, inner, gram)
            pair += 1
    gram = gram.T[0 : gram_send.shape[0]]
    gram_send[...] = gram
    gram_recv[col] = gram

    def gram_copy(j):
        return pltpu.make_async_remote_copy(
            src_ref=gram_send,
            dst_ref=gram_recv.at[col],
            send_sem=gram_ssem.at[j],
            recv_sem=gram_rsem.at[col],
            device_id={"cols": (col + j) % cols},
            device_id_type=MESH,
        )

    for j in range(1, cols):
        gram_copy(j).start()
    for j in range(1, cols):
        src = (col + j) % cols
        pltpu.make_async_remote_copy(
            src_ref=gram_send,
            dst_ref=gram_recv.at[src],
            send_sem=gram_ssem.at[j],
            recv_sem=gram_rsem.at[src],
            device_id={"cols": src},
            device_id_type=MESH,
        ).wait_recv()
    summed = gram_recv[0]
    for c in range(1, cols):
        summed = summed + gram_recv[c]
    inter_ref[...] = (summed * (width * cols) ** (-0.5))[0:pair]

    for j in range(1, n):
        id_copy((me + j) % n).wait_send()
    for c in range(chunks):
        pair_copy(hi, c).wait_send()
        for k in range(far - 2):
            pair_copy(group_of(k), c).wait_send()
            far_copy(group_of(k), c).wait_send()
    for same in (True, False):
        near_copy(same).wait_send()
    for j in range(1, cols):
        gram_copy(j).wait_send()


def body(n, cols, tables, dense_features, slot_rows, slot_examples, slot_counts):
    count, range_rows, width = tables.shape
    here = dense_features.shape[0]
    cap = slot_rows.shape[3]
    far = n // 2
    pairs = (count + 1) * count // 2
    vmem = pl.BlockSpec(memory_space=pltpu.VMEM)
    block = (far, count, here, width)
    chunks = CHUNKS
    any_space = pl.BlockSpec(memory_space=pl.ANY)
    pair_rows = -(-pairs // 8) * 8
    pooled, inter = pl.pallas_call(
        functools.partial(kernel, n, cols),
        out_shape=(
            pltpu.VMEM((here, count, width), jnp.float32),
            pltpu.VMEM((pairs, here), jnp.float32),
        ),
        in_specs=[any_space] * 5,
        out_specs=(vmem, vmem),
        scratch_shapes=[
            pltpu.VMEM((here, width), jnp.float32),
            pltpu.VMEM(slot_rows.shape, jnp.int32),
            pltpu.VMEM(slot_rows.shape, jnp.int32),
            pltpu.SMEM((1, count, n), jnp.int32),
            pltpu.VMEM((count, range_rows, width), jnp.float32),
            pltpu.VMEM((count, range_rows, 2 * width), jnp.bfloat16),
            pltpu.VMEM((n, 2 * count, 2 * cap), jnp.int32),
            pltpu.VMEM((n, 2 * count, 2 * cap), jnp.int32),
            pltpu.VMEM(block, jnp.float32),
            pltpu.VMEM(block, jnp.float32),
            pltpu.VMEM(block, jnp.float32),
            pltpu.VMEM(block, jnp.float32),
            pltpu.VMEM(block, jnp.float32),
            pltpu.VMEM((2,) + block[1:], jnp.float32),
            pltpu.VMEM((cols, pair_rows, here), jnp.float32),
            pltpu.VMEM((pair_rows, here), jnp.float32),
            pltpu.SemaphoreType.DMA((5,)),
            pltpu.SemaphoreType.DMA((n,)),
            pltpu.SemaphoreType.DMA((n,)),
            pltpu.SemaphoreType.DMA((far, chunks)),
            pltpu.SemaphoreType.DMA((far, chunks)),
            pltpu.SemaphoreType.DMA((far, chunks)),
            pltpu.SemaphoreType.DMA((far, chunks)),
            pltpu.SemaphoreType.DMA((2,)),
            pltpu.SemaphoreType.DMA((2,)),
            pltpu.SemaphoreType.DMA((cols,)),
            pltpu.SemaphoreType.DMA((cols,)),
        ],
        compiler_params=pltpu.CompilerParams(collective_id=0, has_side_effects=True),
    )(tables, dense_features, slot_rows, slot_examples, slot_counts.transpose(0, 2, 1))
    return write_out(pooled, inter)


def store(pooled_ref, inter_ref, pooled_hbm, inter_hbm, sem):
    copies = [
        pltpu.make_async_copy(pooled_ref, pooled_hbm, sem.at[0]),
        pltpu.make_async_copy(inter_ref, inter_hbm, sem.at[1]),
    ]
    for copy in copies:
        copy.start()
    for copy in copies:
        copy.wait()


def write_out(pooled, inter):
    vmem = pl.BlockSpec(memory_space=pltpu.VMEM)
    hbm = pl.BlockSpec(memory_space=pl.ANY)
    pooled, inter = pl.pallas_call(
        store,
        out_shape=(
            jax.ShapeDtypeStruct(pooled.shape, pooled.dtype),
            jax.ShapeDtypeStruct(inter.shape, inter.dtype),
        ),
        in_specs=[vmem, vmem],
        out_specs=(hbm, hbm),
        scratch_shapes=[pltpu.SemaphoreType.DMA((2,))],
    )(*(pltpu.with_memory_space_constraint(x, pltpu.VMEM) for x in (pooled, inter)))
    return pooled, inter.T


def solution(mesh):
    placed = (
        P(None, "rows", "cols"),
        P("rows", "cols"),
        P("rows", None, None, None),
        P("rows", None, None, None),
        P("rows", None, None),
    )
    return jax.shard_map(
        functools.partial(body, mesh.shape["rows"], mesh.shape["cols"]),
        mesh=mesh,
        in_specs=placed,
        out_specs=(P("rows", None, "cols"), P("rows", None)),
        check_vma=False,
    )
```

```python
import functools

import jax
import jax.numpy as jnp
from jax import lax
from jax.experimental import pallas as pl
from jax.experimental.pallas import tpu as pltpu
from jax.sharding import PartitionSpec as P

MESH = pl.DeviceIdType.MESH
CHUNKS = 2
DEAD = -65536
OWN, DIRECT, PAIR, FORWARD = range(4)
PLANS = {
    4: (
        ((OWN, 0), (PAIR, 2), (DIRECT, 3), (DIRECT, 1), (FORWARD, 2)),
        ((DIRECT, 0), (OWN, 1), (PAIR, 2), (PAIR, 3), (FORWARD, 2), (FORWARD, 3)),
        ((OWN, 2), (PAIR, 0), (PAIR, 1), (DIRECT, 3), (FORWARD, 0), (FORWARD, 1)),
        ((OWN, 3), (DIRECT, 0), (PAIR, 1), (DIRECT, 2), (FORWARD, 1)),
    )
}
ARRIVALS = {4: ((1, 2, 3), (0, 2, 3), (3, 0, 1), (2, 0, 1))}


def repeat(first, last, step, body):
    if (last - first) // step <= 16:
        for k in range(first, last, step):
            body(k)
    else:
        pl.loop(first, last, step=step)(body)


def kernel(
    n,
    cols,
    fan,
    tables_hbm,
    dense_hbm,
    rows_hbm,
    examples_hbm,
    counts_hbm,
    pooled_ref,
    inter_ref,
    dense_ref,
    rows_ref,
    examples_ref,
    counts_ref,
    table_buf,
    split_buf,
    id_send,
    id_recv,
    id_relay,
    keep,
    cross,
    pair_recv,
    far_send,
    data_recv,
    total_ref,
    gram_recv,
    gram_send,
    load_sem,
    id_ssem,
    id_rsem,
    relay_rsem,
    pair_rsem,
    data_ssem,
    data_rsem,
    gram_ssem,
    gram_rsem,
):
    tables, range_rows, width = table_buf.shape
    here = dense_ref.shape[0]
    cap = rows_ref.shape[3]
    far = n // 2
    chunks = pair_rsem.shape[1]
    step = tables // chunks
    me = lax.axis_index("rows")
    col = lax.axis_index("cols")
    hi, lo = me // 2, me % 2
    mate = hi * 2 + (1 - lo)
    near = hi + 1 - 2 * (hi % 2)
    lead = col // fan * fan + fan - 1
    leads = col == lead

    sources = (counts_hbm, rows_hbm, examples_hbm, tables_hbm, dense_hbm)
    targets = (counts_ref, rows_ref, examples_ref, table_buf, dense_ref)
    loads = [pltpu.make_async_copy(a, b, load_sem.at[i]) for i, (a, b) in enumerate(zip(sources, targets))]

    barrier = pltpu.get_barrier_semaphore()

    def greet(row, at):
        pl.semaphore_signal(barrier, inc=1, device_id={"rows": row, "cols": at}, device_id_type=MESH)

    base = jnp.where(hi == 0, 0, me - 2)

    @pl.when(hi == 0)
    def _():
        greet(2, lead)
        greet(mate, lead)

    repeat(1, n - 2, 1, lambda j: greet(2 + (base + j) % (n - 2), lead))

    @pl.when(jnp.logical_and(hi == 1, leads))
    def _():
        greet(0, col)
        greet(1, col)
        for f in range(1, fan):
            greet(mate, lead - f)

    greet(mate, col)
    for j in range(1, cols):
        greet(me, (col + j) % cols)

    for load in loads:
        load.start()

    slot = lax.broadcasted_iota(jnp.int32, (tables, cap), 1)
    table_id = lax.broadcasted_iota(jnp.int32, (tables, cap), 0)
    for load in loads[:3]:
        load.wait()

    def pack(ref, q, p):
        count = jnp.full((tables, cap), counts_ref[0, 0, p], jnp.int32)
        for t in range(1, tables):
            count = jnp.where(table_id == t, counts_ref[0, t, p], count)
        rows_p = rows_ref[0, p]
        ex_p = jnp.where(slot < count, examples_ref[0, p], DEAD)
        ref[q, 0:tables, :] = jnp.concatenate([rows_p, rows_p], axis=1)
        ref[q, tables : 2 * tables, :] = jnp.concatenate([ex_p, ex_p], axis=1)

    @pl.when(leads)
    def _():
        repeat(0, n, 1, lambda p: pack(id_send, p, p))

    if fan > 1:

        @pl.when(jnp.logical_and(jnp.logical_not(leads), hi == 1))
        def _():
            pack(id_send, mate, mate)

    pack(id_recv, me, me)

    loads[3].wait()
    for t in range(tables):
        whole = table_buf[t]
        high = whole.astype(jnp.bfloat16)
        split_buf[t, :, 0:width] = high
        split_buf[t, :, width : 2 * width] = (whole - high.astype(jnp.float32)).astype(jnp.bfloat16)

    first_half = lax.broadcasted_iota(jnp.int32, (tables, 2 * cap), 1) < cap
    offset = jnp.where(first_half, lo * here, (1 - lo) * here)
    row_iota = lax.broadcasted_iota(jnp.int32, (range_rows, 2 * cap), 0)
    ex_iota = lax.broadcasted_iota(jnp.int32, (2 * here, 2 * cap), 0)

    greeted_lead = jnp.where(hi == 0, cols + fan + 2, cols + fan * (n - 1))
    greeted_rest = jnp.where(hi == 1, cols + 1, cols)
    pl.semaphore_wait(barrier, jnp.where(leads, greeted_lead, greeted_rest))

    def id_copy(src, source, row, at, sem):
        return pltpu.make_async_remote_copy(
            src_ref=src,
            dst_ref=id_recv.at[source],
            send_sem=id_ssem.at[sem],
            recv_sem=id_rsem.at[source],
            device_id={"rows": row, "cols": at},
            device_id_type=MESH,
        )

    def id_wait(source):
        id_copy(id_send.at[source], source, source, lead, 0).wait_recv()

    def relay_copy():
        block = pl.ds(4, n - 4)
        return pltpu.make_async_remote_copy(
            src_ref=id_send.at[block],
            dst_ref=id_relay,
            send_sem=id_ssem.at[2 * fan],
            recv_sem=relay_rsem.at[0],
            device_id={"rows": 2 + lo, "cols": lead},
            device_id_type=MESH,
        )

    def mate_ids(buf, q):
        for f in range(fan):
            id_copy(buf.at[q], me, mate, lead - f, f).start()

    def far_ids():
        def send(j):
            row = (hi + j // 2) % far * 2 + (lo + j) % 2
            for f in reversed(range(fan)):
                id_copy(id_send.at[row], me, row, lead - f, f).start()

        repeat(2, n, 1, send)

    @pl.when(jnp.logical_and(leads, hi == 0))
    def _():
        if n > 4:
            relay_copy().start()
        for row in (2, 3):
            id_copy(id_send.at[row], me, row, lead, 2 * fan).start()
        mate_ids(id_send, mate)

    if fan > 1:

        @pl.when(jnp.logical_and(jnp.logical_not(leads), hi == 1))
        def _():
            mate_ids(id_send, mate)

    @pl.when(jnp.logical_and(leads, hi == 1))
    def _():
        if n > 4:
            relay_copy().wait_recv()

            def relay(j):
                row = n + 3 - j
                for f in reversed(range(fan)):
                    id_copy(id_relay.at[row - 4], lo, row, lead - f, fan + f).start()

            repeat(4, n, 1, relay)
        if fan == 1:
            mate_ids(id_send, mate)
        far_ids()
        for source in (0, 1):
            id_wait(source)
            for f in range(1, fan):
                id_copy(id_recv.at[source], source, me, lead - f, 2 * fan).start()

    @pl.when(jnp.logical_and(leads, hi >= 2))
    def _():
        mate_ids(id_send, mate)
        far_ids()

    def send_block(buf, g, piece, row):
        return pltpu.make_async_remote_copy(
            src_ref=buf.at[g, piece],
            dst_ref=data_recv.at[me, piece],
            send_sem=data_ssem.at[0],
            recv_sem=data_rsem.at[me],
            device_id={"rows": row},
            device_id_type=MESH,
        )

    def data_wait(row):
        pltpu.make_async_remote_copy(
            src_ref=data_recv.at[row],
            dst_ref=data_recv.at[row],
            send_sem=data_ssem.at[0],
            recv_sem=data_rsem.at[row],
            device_id={"rows": row},
            device_id_type=MESH,
        ).wait_recv()

    def pair_copy(g, c):
        piece = pl.ds(c * step, step)
        return pltpu.make_async_remote_copy(
            src_ref=cross.at[g, piece],
            dst_ref=pair_recv.at[g, piece],
            send_sem=data_ssem.at[0],
            recv_sem=pair_rsem.at[g, c],
            device_id={"rows": mate},
            device_id_type=MESH,
        )

    def compute(g, then):
        even = id_recv[g * 2]
        odd = id_recv[g * 2 + 1]
        row_of = jnp.where(first_half, even[0:tables], odd[0:tables])
        code = jnp.where(first_half, even[tables : 2 * tables], odd[tables : 2 * tables]) + offset
        hits = []
        for t in range(tables):
            row_hot = jnp.where(row_iota == row_of[t : t + 1], 1.0, 0.0).astype(jnp.bfloat16)
            ex_hot = jnp.where(ex_iota == code[t : t + 1], 1.0, 0.0).astype(jnp.bfloat16)
            hits.append(
                lax.dot_general(
                    ex_hot, row_hot, (((1,), (1,)), ((), ())), preferred_element_type=jnp.float32
                ).astype(jnp.bfloat16)
            )
        for t in range(tables):
            both = jnp.dot(hits[t], split_buf[t], preferred_element_type=jnp.float32)
            part = both[:, 0:width] + both[:, width : 2 * width]
            keep[g, t] = part[0:here]
            cross[g, t] = part[here : 2 * here]
            if (t + 1) % step == 0:
                then(g, t // step)

    def direct(g, c):
        send_block(keep, g, pl.ds(c * step, step), g * 2 + lo).start()
        send_block(cross, g, pl.ds(c * step, step), g * 2 + 1 - lo).start()

    def own(g, c):
        send_block(cross, g, pl.ds(c * step, step), mate).start()

    def paired(g, c):
        pair_copy(g, c).start()

    def forward(g):
        for c in range(chunks):
            pair_copy(g, c).wait_recv()
            piece = pl.ds(c * step, step)
            far_send[g, piece] = keep[g, piece] + pair_recv[g, piece]
            send_block(far_send, g, piece, g * 2 + lo).start()

    def ids_of(g, hub=False):
        if hub:

            @pl.when(jnp.logical_not(leads))
            def _():
                id_wait(0)
                id_wait(1)
        else:
            id_wait(g * 2)
            id_wait(g * 2 + 1)

    def own_group(g):
        id_wait(mate)
        compute(g, own)

    def group(g, then):
        ids_of(g)
        compute(g, then)

    def add_both(g):
        data_wait(g * 2)
        data_wait(g * 2 + 1)
        total_ref[...] += data_recv[g * 2] + data_recv[g * 2 + 1]

    def add_one(g):
        data_wait(g * 2 + lo)
        total_ref[...] += data_recv[g * 2 + lo]

    def planned(r):
        for op, g in PLANS[far][r]:
            if op == OWN:
                own_group(r)
            elif op == FORWARD:
                forward(g)
            else:
                ids_of(g, r == 1 and g == 0)
                compute(g, direct if op == DIRECT else paired)
        data_wait(mate)
        total_ref[...] = keep[r] + data_recv[mate]
        for g in ARRIVALS[far][r]:
            (add_both if (DIRECT, r) in PLANS[far][g] else add_one)(g)

    def others(action):
        def both(m):
            q = (hi // 2 + m) % (far // 2)
            action(q * 2)
            action(q * 2 + 1)

        repeat(1, far // 2, 1, both)

    def general():
        @pl.when(hi != 1)
        def _():
            own_group(hi)
            group(near, direct)

        @pl.when(hi == 1)
        def _():
            ids_of(0, True)
            compute(0, direct)
            own_group(1)

        others(lambda g: group(g, paired))
        others(forward)
        data_wait(mate)
        total_ref[...] = keep[hi] + data_recv[mate]
        add_both(near)
        others(add_one)

    if far in PLANS:
        for r in range(far):
            pl.when(hi == r)(functools.partial(planned, r))
    else:
        general()

    loads[4].wait()
    vectors = [dense_ref[...]] + [total_ref[t] for t in range(tables)]
    lane = lax.broadcasted_iota(jnp.int32, (here, 128), 1)
    gram = jnp.zeros((here, 128), jnp.float32)
    pair = 0
    for i in range(tables + 1):
        for j in range(i + 1, tables + 1):
            inner = jnp.sum(vectors[i] * vectors[j], axis=1, keepdims=True)
            gram = jnp.where(lane == pair, inner, gram)
            pair += 1
    gram = gram.T[0 : gram_send.shape[0]]
    gram_send[...] = gram

    def gram_copy(source, at):
        return pltpu.make_async_remote_copy(
            src_ref=gram_send,
            dst_ref=gram_recv.at[source],
            send_sem=gram_ssem.at[0],
            recv_sem=gram_rsem.at[source],
            device_id={"cols": at},
            device_id_type=MESH,
        )

    for j in range(1, cols):
        gram_copy(col, (col + j) % cols).start()
    gram_recv[col] = gram
    for t in range(tables):
        pooled_ref[:, t, :] = total_ref[t]
    for j in range(1, cols):
        gram_copy((col + j) % cols, col).wait_recv()
    summed = gram_recv[0]
    for c in range(1, cols):
        summed = summed + gram_recv[c]
    inter_ref[...] = (summed * (width * cols) ** (-0.5))[0:pair]

    def sent(ref, sem):
        pltpu.make_async_remote_copy(
            src_ref=ref,
            dst_ref=ref,
            send_sem=sem,
            recv_sem=gram_rsem.at[0],
            device_id={"rows": mate},
            device_id_type=MESH,
        ).wait_send()

    def ids_sent(tiles, sem):
        sent(id_recv.at[pl.ds(0, tiles)], id_ssem.at[sem])

    sent(data_recv.at[pl.ds(0, n - 1)], data_ssem.at[0])
    sent(gram_recv.at[pl.ds(0, cols - 1)], gram_ssem.at[0])

    @pl.when(jnp.logical_and(leads, hi == 0))
    def _():
        for f in range(fan):
            ids_sent(1, f)
        ids_sent(n - 2, 2 * fan)

    @pl.when(jnp.logical_and(leads, hi >= 2))
    def _():
        for f in range(fan):
            ids_sent(n - 1, f)

    if fan > 1:

        @pl.when(jnp.logical_and(jnp.logical_not(leads), hi == 1))
        def _():
            for f in range(fan):
                ids_sent(1, f)

    @pl.when(jnp.logical_and(leads, hi == 1))
    def _():
        for f in range(fan):
            ids_sent(n - 1 if fan == 1 else n - 2, f)
        if n > 4:
            for f in range(fan):
                ids_sent(n - 4, fan + f)
        if fan > 1:
            ids_sent(2 * (fan - 1), 2 * fan)


def store(pooled_ref, inter_ref, pooled_hbm, inter_hbm, sem):
    copies = [
        pltpu.make_async_copy(pooled_ref, pooled_hbm, sem.at[0]),
        pltpu.make_async_copy(inter_ref, inter_hbm, sem.at[1]),
    ]
    for copy in copies:
        copy.start()
    for copy in copies:
        copy.wait()


def write_out(pooled, inter):
    vmem = pl.BlockSpec(memory_space=pltpu.VMEM)
    hbm = pl.BlockSpec(memory_space=pl.ANY)
    pooled, inter = pl.pallas_call(
        store,
        out_shape=(
            jax.ShapeDtypeStruct(pooled.shape, pooled.dtype),
            jax.ShapeDtypeStruct(inter.shape, inter.dtype),
        ),
        in_specs=[vmem, vmem],
        out_specs=(hbm, hbm),
        scratch_shapes=[pltpu.SemaphoreType.DMA((2,))],
    )(*(pltpu.with_memory_space_constraint(x, pltpu.VMEM) for x in (pooled, inter)))
    return pooled, inter.T


def body(n, cols, tables, dense_features, slot_rows, slot_examples, slot_counts):
    count, range_rows, width = tables.shape
    here = dense_features.shape[0]
    cap = slot_rows.shape[3]
    far = n // 2
    fan = 2 if cols % 2 == 0 else 1
    pairs = (count + 1) * count // 2
    vmem = pl.BlockSpec(memory_space=pltpu.VMEM)
    block = (far, count, here, width)
    chunks = CHUNKS
    any_space = pl.BlockSpec(memory_space=pl.ANY)
    pair_rows = -(-pairs // 8) * 8
    tile = (2 * count, 2 * cap)
    pooled, inter = pl.pallas_call(
        functools.partial(kernel, n, cols, fan),
        out_shape=(
            pltpu.VMEM((here, count, width), jnp.float32),
            pltpu.VMEM((pairs, here), jnp.float32),
        ),
        in_specs=[any_space] * 5,
        out_specs=(vmem, vmem),
        scratch_shapes=[
            pltpu.VMEM((here, width), jnp.float32),
            pltpu.VMEM(slot_rows.shape, jnp.int32),
            pltpu.VMEM(slot_rows.shape, jnp.int32),
            pltpu.SMEM((1, count, n), jnp.int32),
            pltpu.VMEM((count, range_rows, width), jnp.float32),
            pltpu.VMEM((count, range_rows, 2 * width), jnp.bfloat16),
            pltpu.VMEM((n,) + tile, jnp.int32),
            pltpu.VMEM((n,) + tile, jnp.int32),
            pltpu.VMEM((max(n - 4, 1),) + tile, jnp.int32),
            pltpu.VMEM(block, jnp.float32),
            pltpu.VMEM(block, jnp.float32),
            pltpu.VMEM(block, jnp.float32),
            pltpu.VMEM(block, jnp.float32),
            pltpu.VMEM((n,) + block[1:], jnp.float32),
            pltpu.VMEM(block[1:], jnp.float32),
            pltpu.VMEM((cols, pair_rows, here), jnp.float32),
            pltpu.VMEM((pair_rows, here), jnp.float32),
            pltpu.SemaphoreType.DMA((5,)),
            pltpu.SemaphoreType.DMA((2 * fan + 1,)),
            pltpu.SemaphoreType.DMA((n,)),
            pltpu.SemaphoreType.DMA((1,)),
            pltpu.SemaphoreType.DMA((far, chunks)),
            pltpu.SemaphoreType.DMA((1,)),
            pltpu.SemaphoreType.DMA((n,)),
            pltpu.SemaphoreType.DMA((1,)),
            pltpu.SemaphoreType.DMA((cols,)),
        ],
        compiler_params=pltpu.CompilerParams(collective_id=0, has_side_effects=True),
    )(tables, dense_features, slot_rows, slot_examples, slot_counts.transpose(0, 2, 1))
    return write_out(pooled, inter)


def solution(mesh):
    placed = (
        P(None, "rows", "cols"),
        P("rows", "cols"),
        P("rows", None, None, None),
        P("rows", None, None, None),
        P("rows", None, None),
    )
    return jax.shard_map(
        functools.partial(body, mesh.shape["rows"], mesh.shape["cols"]),
        mesh=mesh,
        in_specs=placed,
        out_specs=(P("rows", None, "cols"), P("rows", None)),
        check_vma=False,
    )
```

```python
import functools

import jax
import jax.numpy as jnp
from jax import lax
from jax.experimental import pallas as pl
from jax.experimental.pallas import tpu as pltpu
from jax.sharding import PartitionSpec as P

MESH = pl.DeviceIdType.MESH
CHUNKS = 4
BLOCKS = 2
DEAD = -65536
OWN, DIRECT, PAIR, MIXED, FORWARD = range(5)
PLANS = {
    4: (
        ((OWN, 0), (PAIR, 2), (MIXED, 3), (DIRECT, 1), (FORWARD, 2), (FORWARD, 3)),
        ((DIRECT, 0), (PAIR, 2), (PAIR, 3), (OWN, 1), (FORWARD, 2), (FORWARD, 3)),
        ((OWN, 2), (PAIR, 0), (PAIR, 1), (DIRECT, 3), (FORWARD, 0), (FORWARD, 1)),
        ((OWN, 3), (DIRECT, 0), (PAIR, 1), (DIRECT, 2), (FORWARD, 1)),
    )
}
ARRIVALS = {4: ((1, 2, 3), (0, 2, 3), (3, 0, 1), (2, 0, 1))}


def repeat(first, last, step, body):
    if (last - first) // step <= 16:
        for k in range(first, last, step):
            body(k)
    else:
        pl.loop(first, last, step=step)(body)


def kernel(
    n,
    cols,
    fan,
    tables_hbm,
    dense_hbm,
    rows_hbm,
    examples_hbm,
    counts_hbm,
    pooled_ref,
    inter_ref,
    dense_ref,
    slots_ref,
    counts_ref,
    table_buf,
    split_buf,
    ids,
    keep,
    cross,
    pair_recv,
    far_send,
    data_recv,
    total_ref,
    gram_recv,
    gram_send,
    load_sem,
    id_ssem,
    id_rsem,
    relay_rsem,
    pair_rsem,
    data_ssem,
    data_rsem,
    gram_ssem,
    gram_rsem,
):
    tables, range_rows, width = table_buf.shape
    here = dense_ref.shape[0]
    cap = slots_ref.shape[4]
    far = n // 2
    chunks = pair_rsem.shape[1]
    step = tables // chunks
    me = lax.axis_index("rows")
    col = lax.axis_index("cols")
    hi, lo = me // 2, me % 2
    mate = hi * 2 + (1 - lo)
    near = hi + 1 - 2 * (hi % 2)
    lead = col // fan * fan + fan - 1
    leads = col == lead
    id_send, id_recv, id_relay = ids.at[pl.ds(0, n)], ids.at[pl.ds(n, n)], ids.at[pl.ds(2 * n, max(n - 4, 1))]
    early = lead - fan + 1

    loads = [
        pltpu.make_async_copy(source, target, load_sem.at[i])
        for source, target, i in (
            (counts_hbm, counts_ref, 0),
            (rows_hbm, slots_ref.at[0], 1),
            (examples_hbm, slots_ref.at[1], 1),
            (tables_hbm, table_buf, 2),
            (dense_hbm, dense_ref, 3),
        )
    ]

    barrier = pltpu.get_barrier_semaphore()

    def greet(row, at):
        pl.semaphore_signal(barrier, inc=1, device_id={"rows": row, "cols": at}, device_id_type=MESH)

    @pl.when(hi == 0)
    def _():
        greet(2, early)
        greet(3, early)
        greet(mate, lead)
        repeat(4, n, 1, lambda row: greet(row, lead))

    @pl.when(hi >= 1)
    def _():
        repeat(1, n - 2, 1, lambda j: greet(2 + (me - 2 + j) % (n - 2), lead))

    @pl.when(jnp.logical_and(hi == 1, leads))
    def _():
        greet(0, col)
        greet(1, col)
        for f in range(1, fan):
            greet(mate, lead - f)

    greet(mate, col)
    for j in range(1, cols):
        greet(me, (col + j) % cols)

    for load in loads:
        load.start()

    slot = lax.broadcasted_iota(jnp.int32, (tables, cap), 1)
    table_id = lax.broadcasted_iota(jnp.int32, (tables, cap), 0)
    loads[0].wait()
    pltpu.make_async_copy(slots_ref, slots_ref, load_sem.at[1]).wait()

    def pack(ref, q, p):
        count = jnp.full((tables, cap), counts_ref[0, 0, p], jnp.int32)
        for t in range(1, tables):
            count = jnp.where(table_id == t, counts_ref[0, t, p], count)
        rows_p = slots_ref[0, 0, p]
        ex_p = jnp.where(slot < count, slots_ref[1, 0, p], DEAD)
        ref[q, 0:tables, :] = jnp.concatenate([rows_p, rows_p], axis=1)
        ref[q, tables : 2 * tables, :] = jnp.concatenate([ex_p, ex_p], axis=1)

    @pl.when(leads)
    def _():
        repeat(0, n, 1, lambda p: pack(id_send, p, p))

    if fan > 1:

        @pl.when(jnp.logical_and(jnp.logical_not(leads), hi == 1))
        def _():
            for row in (mate, 0, 1):
                pack(id_send, row, row)

    pack(id_recv, me, me)

    loads[3].wait()
    for t in range(tables):
        whole = table_buf[t]
        high = whole.astype(jnp.bfloat16)
        split_buf[t, :, 0:width] = high
        split_buf[t, :, width : 2 * width] = (whole - high.astype(jnp.float32)).astype(jnp.bfloat16)

    first_half = lax.broadcasted_iota(jnp.int32, (tables, 2 * cap), 1) < cap
    offset = jnp.where(first_half, lo * here, (1 - lo) * here)
    row_iota = lax.broadcasted_iota(jnp.int32, (range_rows, 2 * cap), 0)
    ex_iota = lax.broadcasted_iota(jnp.int32, (2 * here, 2 * cap), 0)

    greeted_lead = cols + fan * (n - 1)
    greeted_lead = jnp.where(hi == 0, cols + fan + 2, greeted_lead)
    greeted_lead = jnp.where(hi == 1, cols + fan * (n - 3) + (2 if fan == 1 else 0), greeted_lead)
    greeted_rest = jnp.where(hi == 1, cols + 1 + 2 * fan, cols)
    pl.semaphore_wait(barrier, jnp.where(leads, greeted_lead, greeted_rest))

    def id_copy(src, source, row, at):
        return pltpu.make_async_remote_copy(
            src_ref=src,
            dst_ref=id_recv.at[source],
            send_sem=id_ssem.at[0],
            recv_sem=id_rsem.at[source // 2],
            device_id={"rows": row, "cols": at},
            device_id_type=MESH,
        )

    def ids_wait(first, tiles):
        block = id_recv.at[pl.ds(first, tiles)]
        pltpu.make_async_remote_copy(
            src_ref=block,
            dst_ref=block,
            send_sem=id_ssem.at[0],
            recv_sem=id_rsem.at[first // 2],
            device_id={"rows": mate},
            device_id_type=MESH,
        ).wait_recv()

    def relay_copy():
        block = pl.ds(4, n - 4)
        return pltpu.make_async_remote_copy(
            src_ref=id_send.at[block],
            dst_ref=id_relay,
            send_sem=id_ssem.at[0],
            recv_sem=relay_rsem.at[0],
            device_id={"rows": 2 + lo, "cols": lead},
            device_id_type=MESH,
        )

    def ids_to(row):
        for f in reversed(range(fan)):
            id_copy(id_send.at[row], me, row, lead - f).start()

    def far_ids(last):
        repeat(2, last, 1, lambda j: ids_to((hi + j // 2) % far * 2 + (lo + j) % 2))

    @pl.when(jnp.logical_and(leads, hi == 0))
    def _():
        if n > 4:
            relay_copy().start()
        for row in (2, 3):
            id_copy(id_send.at[row], me, row, lead).start()
        ids_to(mate)

    @pl.when(jnp.logical_and(col == early, hi == 1))
    def _():
        for row in (mate, 0, 1):
            ids_to(row)

    @pl.when(jnp.logical_and(leads, hi == 1))
    def _():
        if n > 4:
            relay_copy().wait_recv()

            def relay(j):
                row = n + 3 - j
                for f in reversed(range(fan)):
                    id_copy(id_relay.at[row - 4], lo, row, lead - f).start()

            repeat(4, n, 1, relay)
        far_ids(n - 2)
        ids_wait(0, 2)
        for f in range(1, fan):
            for source in (0, 1):
                id_copy(id_recv.at[source], source, me, lead - f).start()

    @pl.when(jnp.logical_and(leads, hi >= 2))
    def _():
        ids_to(mate)
        far_ids(n)

    def send_block(buf, g, piece, row):
        return pltpu.make_async_remote_copy(
            src_ref=buf.at[g, piece],
            dst_ref=data_recv.at[pl.ds(me * tables + piece.start, piece.size)],
            send_sem=data_ssem.at[0],
            recv_sem=data_rsem.at[hi],
            device_id={"rows": row},
            device_id_type=MESH,
        )

    def slot_of(row):
        return pl.ds(row * tables, tables)

    def data_wait(g, first, blocks):
        block = data_recv.at[pl.ds(first, blocks)]
        pltpu.make_async_remote_copy(
            src_ref=block,
            dst_ref=block,
            send_sem=data_ssem.at[0],
            recv_sem=data_rsem.at[g],
            device_id={"rows": mate},
            device_id_type=MESH,
        ).wait_recv()

    def pair_copy(g, c):
        piece = pl.ds(c * step, step)
        return pltpu.make_async_remote_copy(
            src_ref=cross.at[g, piece],
            dst_ref=pair_recv.at[g, piece],
            send_sem=data_ssem.at[0],
            recv_sem=pair_rsem.at[(g - hi - 1) % far, c],
            device_id={"rows": mate},
            device_id_type=MESH,
        )

    def compute(g, then):
        even = id_recv[g * 2]
        odd = id_recv[g * 2 + 1]
        row_of = jnp.where(first_half, even[0:tables], odd[0:tables])
        code = jnp.where(first_half, even[tables : 2 * tables], odd[tables : 2 * tables]) + offset
        def count(t):
            row_hot = jnp.where(row_iota == row_of[t : t + 1], 1.0, 0.0).astype(jnp.bfloat16)
            ex_hot = jnp.where(ex_iota == code[t : t + 1], 1.0, 0.0).astype(jnp.bfloat16)
            return lax.dot_general(
                ex_hot, row_hot, (((1,), (1,)), ((), ())), preferred_element_type=jnp.float32
            ).astype(jnp.bfloat16)

        def look_up(t, hits):
            both = jnp.dot(hits, split_buf[t], preferred_element_type=jnp.float32)
            return both[:, 0:width] + both[:, width : 2 * width]

        hits = [count(t) for t in range(tables)]
        parts = [look_up(t, hits[t]) for t in range(tables)]
        for t in range(tables):
            keep[g, t] = parts[t][0:here]
            cross[g, t] = parts[t][here : 2 * here]
            if (t + 1) % step == 0:
                then(g, t // step)

    span = tables // BLOCKS

    def pieces(c):
        last = (c + 1) * step
        return [pl.ds(last - span, span)] if last % span == 0 else []

    def direct(g, c):
        for piece in pieces(c):
            send_block(keep, g, piece, g * 2 + lo).start()
            send_block(cross, g, piece, g * 2 + 1 - lo).start()

    def own(g, c):
        for piece in pieces(c):
            send_block(cross, g, piece, mate).start()

    def paired(g, c):
        pair_copy(g, c).start()

    def forward(g, some):
        for c in range(some):
            pair_copy(g, c).wait_recv()
            piece = pl.ds(c * step, step)
            far_send[g, piece] = keep[g, piece] + pair_recv[g, piece]
            send_block(far_send, g, piece, g * 2 + lo).start()

    def mixed(g, c):
        (direct if c >= chunks // 2 else paired)(g, c)

    def ids_of(g, hub=False):
        if hub:
            pl.when(jnp.logical_not(leads))(lambda: ids_wait(g * 2, 2))
        else:
            ids_wait(g * 2, 2)

    def own_group(g):
        ids_wait(mate, 1)
        compute(g, own)

    def add_own(g):
        data_wait(g, mate * tables, tables)
        total_ref[...] = keep[g] + data_recv[slot_of(mate)]

    def add_direct(g):
        data_wait(g, 2 * g * tables, 2 * tables)
        total_ref[...] += data_recv[slot_of(2 * g)] + data_recv[slot_of(2 * g + 1)]

    def add_paired(g):
        data_wait(g, (2 * g + lo) * tables, tables)
        total_ref[...] += data_recv[slot_of(2 * g + lo)]

    def add_mixed(g):
        late = tables // 2
        data_wait(g, 2 * g * tables, tables + late)
        total_ref[...] += data_recv[slot_of(2 * g + lo)]
        total_ref[late:] += data_recv[pl.ds((2 * g + 1 - lo) * tables + late, late)]

    def planned(r):
        sends = {DIRECT: direct, PAIR: paired, MIXED: mixed}
        adds = {DIRECT: add_direct, PAIR: add_paired, MIXED: add_mixed}
        plan = PLANS[far][r]
        for op, g in plan:
            if op == OWN:
                own_group(r)
            elif op == FORWARD:
                forward(g, chunks // 2 if (MIXED, g) in plan else chunks)
            else:
                ids_of(g, r == 1 and g == 0)
                compute(g, sends[op])
        add_own(r)
        for g in ARRIVALS[far][r]:
            adds[next(op for op, to in PLANS[far][g] if op in adds and to == r)](g)

    def others(action):
        def both(m):
            q = (hi // 2 + m) % (far // 2)
            action(q * 2)
            action(q * 2 + 1)

        repeat(1, far // 2, 1, both)

    def general():
        @pl.when(hi != 1)
        def _():
            own_group(hi)
            ids_of(near)
            compute(near, direct)

        @pl.when(hi == 1)
        def _():
            ids_of(0, True)
            compute(0, direct)
            own_group(1)

        def far_group(g):
            ids_of(g)
            compute(g, paired)

        others(far_group)
        others(lambda g: forward(g, chunks))
        add_own(hi)
        add_direct(near)
        others(add_paired)

    if far in PLANS:
        for r in range(far):
            pl.when(hi == r)(functools.partial(planned, r))
    else:
        general()

    loads[4].wait()
    vectors = [dense_ref[...]] + [total_ref[t] for t in range(tables)]
    lane = lax.broadcasted_iota(jnp.int32, (here, 128), 1)
    gram = jnp.zeros((here, 128), jnp.float32)
    pair = 0
    for i in range(tables + 1):
        for j in range(i + 1, tables + 1):
            inner = jnp.sum(vectors[i] * vectors[j], axis=1, keepdims=True)
            gram = jnp.where(lane == pair, inner, gram)
            pair += 1
    gram = gram.T[0 : gram_send.shape[0]]
    gram_send[...] = gram

    def gram_copy(source, at):
        return pltpu.make_async_remote_copy(
            src_ref=gram_send,
            dst_ref=gram_recv.at[source],
            send_sem=gram_ssem.at[0],
            recv_sem=gram_rsem.at[0],
            device_id={"cols": at},
            device_id_type=MESH,
        )

    for j in range(1, cols):
        gram_copy(col, (col + j) % cols).start()
    gram_recv[col] = gram
    for t in range(tables):
        pooled_ref[:, t, :] = total_ref[t]
    block = gram_recv.at[pl.ds(0, cols - 1)]
    pltpu.make_async_remote_copy(
        src_ref=block,
        dst_ref=block,
        send_sem=gram_ssem.at[0],
        recv_sem=gram_rsem.at[0],
        device_id={"rows": mate},
        device_id_type=MESH,
    ).wait_recv()
    summed = gram_recv[0]
    for c in range(1, cols):
        summed = summed + gram_recv[c]
    inter_ref[...] = (summed * (width * cols) ** (-0.5))[0:pair]

    def sent(ref, sem):
        pltpu.make_async_remote_copy(
            src_ref=ref,
            dst_ref=ref,
            send_sem=sem,
            recv_sem=gram_rsem.at[0],
            device_id={"rows": mate},
            device_id_type=MESH,
        ).wait_send()

    sent(data_recv.at[pl.ds(0, (n - 1) * tables)], data_ssem.at[0])
    sent(gram_recv.at[pl.ds(0, cols - 1)], gram_ssem.at[0])

    far_sent = fan * (n - 4)
    hub_sent = far_sent + (far_sent + 2 * (fan - 1) if fan > 1 else n - 1)

    def ids_sent(when, tiles):
        @pl.when(when)
        def _():
            sent(ids.at[pl.ds(0, tiles)], id_ssem.at[0])

    ids_sent(jnp.logical_and(leads, hi == 0), fan + n - 2)
    ids_sent(jnp.logical_and(leads, hi == 1), hub_sent)
    ids_sent(jnp.logical_and(leads, hi >= 2), fan * (n - 1))
    if fan > 1:
        ids_sent(jnp.logical_and(col == early, hi == 1), 3 * fan)


def store(pooled_ref, inter_ref, pooled_hbm, inter_hbm, sem):
    copies = [
        pltpu.make_async_copy(pooled_ref, pooled_hbm, sem.at[0]),
        pltpu.make_async_copy(inter_ref, inter_hbm, sem.at[1]),
    ]
    for copy in copies:
        copy.start()
    for copy in copies:
        copy.wait()


def write_out(pooled, inter):
    vmem = pl.BlockSpec(memory_space=pltpu.VMEM)
    hbm = pl.BlockSpec(memory_space=pl.ANY)
    pooled, inter = pl.pallas_call(
        store,
        out_shape=(
            jax.ShapeDtypeStruct(pooled.shape, pooled.dtype),
            jax.ShapeDtypeStruct(inter.shape, inter.dtype),
        ),
        in_specs=[vmem, vmem],
        out_specs=(hbm, hbm),
        scratch_shapes=[pltpu.SemaphoreType.DMA((2,))],
    )(*(pltpu.with_memory_space_constraint(x, pltpu.VMEM) for x in (pooled, inter)))
    return pooled, inter.T


def body(n, cols, tables, dense_features, slot_rows, slot_examples, slot_counts):
    count, range_rows, width = tables.shape
    here = dense_features.shape[0]
    cap = slot_rows.shape[3]
    far = n // 2
    fan = 2 if cols % 2 == 0 else 1
    pairs = (count + 1) * count // 2
    vmem = pl.BlockSpec(memory_space=pltpu.VMEM)
    block = (far, count, here, width)
    chunks = CHUNKS
    any_space = pl.BlockSpec(memory_space=pl.ANY)
    pair_rows = -(-pairs // 8) * 8
    tile = (2 * count, 2 * cap)
    pooled, inter = pl.pallas_call(
        functools.partial(kernel, n, cols, fan),
        out_shape=(
            pltpu.VMEM((here, count, width), jnp.float32),
            pltpu.VMEM((pairs, here), jnp.float32),
        ),
        in_specs=[any_space] * 5,
        out_specs=(vmem, vmem),
        scratch_shapes=[
            pltpu.VMEM((here, width), jnp.float32),
            pltpu.VMEM((2,) + slot_rows.shape, jnp.int32),
            pltpu.SMEM((1, count, n), jnp.int32),
            pltpu.VMEM((count, range_rows, width), jnp.float32),
            pltpu.VMEM((count, range_rows, 2 * width), jnp.bfloat16),
            pltpu.VMEM((4 * n,) + tile, jnp.int32),
            pltpu.VMEM(block, jnp.float32),
            pltpu.VMEM(block, jnp.float32),
            pltpu.VMEM(block, jnp.float32),
            pltpu.VMEM(block, jnp.float32),
            pltpu.VMEM((n * count,) + block[2:], jnp.float32),
            pltpu.VMEM(block[1:], jnp.float32),
            pltpu.VMEM((cols, pair_rows, here), jnp.float32),
            pltpu.VMEM((pair_rows, here), jnp.float32),
            pltpu.SemaphoreType.DMA((4,)),
            pltpu.SemaphoreType.DMA((1,)),
            pltpu.SemaphoreType.DMA((far,)),
            pltpu.SemaphoreType.DMA((1,)),
            pltpu.SemaphoreType.DMA((far - 1, chunks)),
            pltpu.SemaphoreType.DMA((1,)),
            pltpu.SemaphoreType.DMA((far,)),
            pltpu.SemaphoreType.DMA((1,)),
            pltpu.SemaphoreType.DMA((1,)),
        ],
        compiler_params=pltpu.CompilerParams(collective_id=0, has_side_effects=True),
    )(tables, dense_features, slot_rows, slot_examples, slot_counts.transpose(0, 2, 1))
    return write_out(pooled, inter)


def solution(mesh):
    placed = (
        P(None, "rows", "cols"),
        P("rows", "cols"),
        P("rows", None, None, None),
        P("rows", None, None, None),
        P("rows", None, None),
    )
    return jax.shard_map(
        functools.partial(body, mesh.shape["rows"], mesh.shape["cols"]),
        mesh=mesh,
        in_specs=placed,
        out_specs=(P("rows", None, "cols"), P("rows", None)),
        check_vma=False,
    )
```

```python
import functools

import jax
import jax.numpy as jnp
from jax import lax
from jax.experimental import pallas as pl
from jax.experimental.pallas import tpu as pltpu
from jax.sharding import PartitionSpec as P

MESH = pl.DeviceIdType.MESH
CHUNKS = 4
BLOCKS = 2
DEAD = -65536
OWN, DIRECT, PAIR, FORWARD = range(4)
PLANS = {
    4: (
        ((OWN, 0), (PAIR, 2), (PAIR, 3), (DIRECT, 1), (FORWARD, 2), (FORWARD, 3)),
        ((DIRECT, 0), (PAIR, 2), (PAIR, 3), (OWN, 1), (FORWARD, 2), (FORWARD, 3)),
        ((OWN, 2), (PAIR, 0), (PAIR, 1), (DIRECT, 3), (FORWARD, 0), (FORWARD, 1)),
        ((OWN, 3), (DIRECT, 0), (PAIR, 1), (DIRECT, 2), (FORWARD, 1)),
    )
}
ARRIVALS = {4: ((1, 2, 3), (0, 2, 3), (3, 0, 1), (2, 0, 1))}


def repeat(first, last, step, body):
    if (last - first) // step <= 16:
        for k in range(first, last, step):
            body(k)
    else:
        pl.loop(first, last, step=step)(body)


def kernel(
    n,
    cols,
    fan,
    tables_hbm,
    dense_hbm,
    rows_hbm,
    examples_hbm,
    counts_hbm,
    pooled_ref,
    inter_ref,
    dense_ref,
    slots_ref,
    counts_ref,
    table_buf,
    split_buf,
    ids,
    keep,
    cross,
    pair_recv,
    far_send,
    data_recv,
    total_ref,
    gram_recv,
    gram_send,
    load_sem,
    id_ssem,
    id_rsem,
    relay_rsem,
    pair_rsem,
    data_ssem,
    data_rsem,
    gram_ssem,
    gram_rsem,
    ready_sem,
):
    tables, range_rows, width = table_buf.shape
    here = dense_ref.shape[0]
    cap = slots_ref.shape[4]
    far = n // 2
    chunks = pair_rsem.shape[1]
    step = tables // chunks
    me = lax.axis_index("rows")
    col = lax.axis_index("cols")
    hi, lo = me // 2, me % 2
    mate = hi * 2 + (1 - lo)
    near = hi + 1 - 2 * (hi % 2)
    lead = col // fan * fan + fan - 1
    leads = col == lead
    id_send, id_recv, id_relay = ids.at[pl.ds(0, n)], ids.at[pl.ds(n, n)], ids.at[pl.ds(2 * n, max(n - 4, 1))]
    early = lead - fan + 1

    loads = [
        pltpu.make_async_copy(source, target, load_sem.at[i])
        for source, target, i in (
            (counts_hbm, counts_ref, 0),
            (rows_hbm, slots_ref.at[0], 1),
            (examples_hbm, slots_ref.at[1], 1),
            (tables_hbm, table_buf, 2),
            (dense_hbm, dense_ref, 3),
        )
    ]

    barrier = pltpu.get_barrier_semaphore()

    def greet(row, at):
        pl.semaphore_signal(barrier, inc=1, device_id={"rows": row, "cols": at}, device_id_type=MESH)

    @pl.when(hi == 0)
    def _():
        greet(2, early)
        greet(3, early)
        greet(mate, lead)
        repeat(4, n, 1, lambda row: greet(row, lead))

    @pl.when(hi >= 1)
    def _():
        repeat(1, n - 2, 1, lambda j: greet(2 + (me - 2 + j) % (n - 2), lead))

    @pl.when(jnp.logical_and(hi == 1, leads))
    def _():
        greet(0, col)
        greet(1, col)
        for f in range(1, fan):
            greet(mate, lead - f)

    greet(mate, col)
    for c in range(1, cols):
        pl.when(col < c)(functools.partial(greet, me, c))

    for load in loads:
        load.start()

    slot = lax.broadcasted_iota(jnp.int32, (tables, cap), 1)
    half = lax.broadcasted_iota(jnp.int32, (tables, 2 * cap), 1) // cap
    table_id = lax.broadcasted_iota(jnp.int32, (tables, cap), 0)
    loads[0].wait()
    pltpu.make_async_copy(slots_ref, slots_ref, load_sem.at[1]).wait()

    def pack(ref, q, p):
        count = jnp.full((tables, cap), counts_ref[0, 0, p], jnp.int32)
        for t in range(1, tables):
            count = jnp.where(table_id == t, counts_ref[0, t, p], count)
        rows_p = slots_ref[0, 0, p]
        ex_p = jnp.where(slot < count, slots_ref[1, 0, p], DEAD)
        rows_p = jnp.concatenate([rows_p, rows_p], axis=1)
        ref[q] = jnp.where(half == lo, rows_p, jnp.concatenate([ex_p, ex_p], axis=1))

    @pl.when(leads)
    def _():
        repeat(0, n, 1, lambda p: pack(id_send, p, p))

    if fan > 1:

        @pl.when(jnp.logical_and(jnp.logical_not(leads), hi == 1))
        def _():
            for row in (mate, 0, 1):
                pack(id_send, row, row)

    pack(id_recv, me, me)

    loads[3].wait()
    for t in range(tables):
        whole = table_buf[t]
        high = whole.astype(jnp.bfloat16)
        split_buf[t, :, 0:width] = high
        split_buf[t, :, width : 2 * width] = (whole - high.astype(jnp.float32)).astype(jnp.bfloat16)

    first_half = half == 0
    offset = jnp.where(first_half, lo * here, (1 - lo) * here)
    row_iota = lax.broadcasted_iota(jnp.int32, (range_rows, 2 * cap), 0)
    ex_iota = lax.broadcasted_iota(jnp.int32, (2 * here, 2 * cap), 0)

    greeted_lead = col + 1 + fan * (n - 1)
    greeted_lead = jnp.where(hi == 0, col + fan + 3, greeted_lead)
    greeted_lead = jnp.where(hi == 1, col + 1 + fan * (n - 3) + (2 if fan == 1 else 0), greeted_lead)
    greeted_rest = jnp.where(hi == 1, col + 2 + 2 * fan, col + 1)
    pl.semaphore_wait(barrier, jnp.where(leads, greeted_lead, greeted_rest))

    def answer(at):
        pl.semaphore_signal(ready_sem, inc=1, device_id={"cols": at}, device_id_type=MESH)

    def id_copy(src, source, row, at):
        return pltpu.make_async_remote_copy(
            src_ref=src,
            dst_ref=id_recv.at[source],
            send_sem=id_ssem.at[0],
            recv_sem=id_rsem.at[source // 2],
            device_id={"rows": row, "cols": at},
            device_id_type=MESH,
        )

    def ids_wait(first, tiles):
        block = id_recv.at[pl.ds(first, tiles)]
        pltpu.make_async_remote_copy(
            src_ref=block,
            dst_ref=block,
            send_sem=id_ssem.at[0],
            recv_sem=id_rsem.at[first // 2],
            device_id={"rows": mate},
            device_id_type=MESH,
        ).wait_recv()

    def relay_copy():
        block = pl.ds(4, n - 4)
        return pltpu.make_async_remote_copy(
            src_ref=id_send.at[block],
            dst_ref=id_relay,
            send_sem=id_ssem.at[0],
            recv_sem=relay_rsem.at[0],
            device_id={"rows": 2 + lo, "cols": lead},
            device_id_type=MESH,
        )

    def ids_to(row):
        for f in reversed(range(fan)):
            id_copy(id_send.at[row], me, row, lead - f).start()

    def far_ids(first):
        def to(j):
            g = j // 2
            ids_to(jnp.where(g >= hi, g + 1, g) * 2 + (lo + j) % 2)

        repeat(first, n - 2, 1, to)

    @pl.when(jnp.logical_and(leads, hi == 0))
    def _():
        if n > 4:
            relay_copy().start()
        for row in (2, 3):
            id_copy(id_send.at[row], me, row, lead).start()
        ids_to(mate)

    @pl.when(jnp.logical_and(col == early, hi == 1))
    def _():
        for row in (mate, 0, 1):
            ids_to(row)

    @pl.when(jnp.logical_and(leads, hi == 1))
    def _():
        if n > 4:
            relay_copy().wait_recv()

            def relay(j):
                row = n + 3 - j
                for f in reversed(range(fan)):
                    id_copy(id_relay.at[row - 4], lo, row, lead - f).start()

            repeat(4, n, 1, relay)
        far_ids(2)
        ids_wait(0, 2)
        for f in range(1, fan):
            for source in (0, 1):
                id_copy(id_recv.at[source], source, me, lead - f).start()

    @pl.when(jnp.logical_and(leads, hi >= 2))
    def _():
        ids_to(mate)
        far_ids(0)

    for c in range(cols - 1):
        pl.when(col > c)(functools.partial(answer, c))

    def send_block(buf, g, piece, row):
        return pltpu.make_async_remote_copy(
            src_ref=buf.at[g, piece],
            dst_ref=data_recv.at[pl.ds(me * tables + piece.start, piece.size)],
            send_sem=data_ssem.at[0],
            recv_sem=data_rsem.at[hi],
            device_id={"rows": row},
            device_id_type=MESH,
        )

    def slot_of(row):
        return pl.ds(row * tables, tables)

    def data_wait(g, first, blocks):
        block = data_recv.at[pl.ds(first, blocks)]
        pltpu.make_async_remote_copy(
            src_ref=block,
            dst_ref=block,
            send_sem=data_ssem.at[0],
            recv_sem=data_rsem.at[g],
            device_id={"rows": mate},
            device_id_type=MESH,
        ).wait_recv()

    def pair_copy(g, c):
        piece = pl.ds(c * step, step)
        return pltpu.make_async_remote_copy(
            src_ref=cross.at[g, piece],
            dst_ref=pair_recv.at[g, piece],
            send_sem=data_ssem.at[0],
            recv_sem=pair_rsem.at[(g - hi - 1) % far, c],
            device_id={"rows": mate},
            device_id_type=MESH,
        )

    def compute(g, then):
        even = id_recv[g * 2]
        odd = id_recv[g * 2 + 1]
        row_of = jnp.where(first_half, even, odd)
        code = jnp.where(first_half, odd, even)
        code = jnp.concatenate([code[:, cap:], code[:, :cap]], axis=1) + offset
        def count(t):
            row_hot = jnp.where(row_iota == row_of[t : t + 1], 1.0, 0.0).astype(jnp.bfloat16)
            ex_hot = jnp.where(ex_iota == code[t : t + 1], 1.0, 0.0).astype(jnp.bfloat16)
            return lax.dot_general(
                ex_hot, row_hot, (((1,), (1,)), ((), ())), preferred_element_type=jnp.float32
            ).astype(jnp.bfloat16)

        def look_up(t, hits):
            both = jnp.dot(hits, split_buf[t], preferred_element_type=jnp.float32)
            return both[:, 0:width] + both[:, width : 2 * width]

        hits = [count(t) for t in range(tables)]
        parts = [look_up(t, hits[t]) for t in range(tables)]
        for t in range(tables):
            keep[g, t] = parts[t][0:here]
            cross[g, t] = parts[t][here : 2 * here]
            if (t + 1) % step == 0:
                then(g, t // step)

    span = tables // BLOCKS

    def pieces(c):
        last = (c + 1) * step
        return [pl.ds(last - span, span)] if last % span == 0 else []

    def direct(g, c):
        for piece in pieces(c):
            send_block(keep, g, piece, g * 2 + lo).start()
            send_block(cross, g, piece, g * 2 + 1 - lo).start()

    def own(g, c):
        for piece in pieces(c):
            send_block(cross, g, piece, mate).start()

    def paired(g, c):
        pair_copy(g, c).start()

    def forward(g):
        for c in range(chunks):
            pair_copy(g, c).wait_recv()
            piece = pl.ds(c * step, step)
            far_send[g, piece] = keep[g, piece] + pair_recv[g, piece]
            send_block(far_send, g, piece, g * 2 + lo).start()

    def ids_of(g, hub=False):
        if hub:
            pl.when(jnp.logical_not(leads))(lambda: ids_wait(g * 2, 2))
        else:
            ids_wait(g * 2, 2)

    def own_group(g):
        ids_wait(mate, 1)
        compute(g, own)

    def add_own(g):
        data_wait(g, mate * tables, tables)
        total_ref[...] = keep[g] + data_recv[slot_of(mate)]

    def add_direct(g):
        data_wait(g, 2 * g * tables, 2 * tables)
        total_ref[...] += data_recv[slot_of(2 * g)] + data_recv[slot_of(2 * g + 1)]

    def add_paired(g):
        data_wait(g, (2 * g + lo) * tables, tables)
        total_ref[...] += data_recv[slot_of(2 * g + lo)]

    def planned(r):
        sends = {DIRECT: direct, PAIR: paired}
        adds = {DIRECT: add_direct, PAIR: add_paired}
        for op, g in PLANS[far][r]:
            if op == OWN:
                own_group(r)
            elif op == FORWARD:
                forward(g)
            else:
                ids_of(g, r == 1 and g == 0)
                compute(g, sends[op])
        add_own(r)
        for g in ARRIVALS[far][r]:
            adds[DIRECT if (DIRECT, r) in PLANS[far][g] else PAIR](g)

    def others(action):
        def both(m):
            q = (hi // 2 + m) % (far // 2)
            action(q * 2)
            action(q * 2 + 1)

        repeat(1, far // 2, 1, both)

    def general():
        @pl.when(hi != 1)
        def _():
            own_group(hi)
            ids_of(near)
            compute(near, direct)

        @pl.when(hi == 1)
        def _():
            ids_of(0, True)
            compute(0, direct)
            own_group(1)

        def far_group(g):
            ids_of(g)
            compute(g, paired)

        others(far_group)
        others(forward)
        add_own(hi)
        add_direct(near)
        others(add_paired)

    if far in PLANS:
        for r in range(far):
            pl.when(hi == r)(functools.partial(planned, r))
    else:
        general()

    loads[4].wait()
    vectors = [dense_ref[...]] + [total_ref[t] for t in range(tables)]
    lane = lax.broadcasted_iota(jnp.int32, (here, 128), 1)
    gram = jnp.zeros((here, 128), jnp.float32)
    pair = 0
    for i in range(tables + 1):
        for j in range(i + 1, tables + 1):
            inner = jnp.sum(vectors[i] * vectors[j], axis=1, keepdims=True)
            gram = jnp.where(lane == pair, inner, gram)
            pair += 1
    gram = gram.T[0 : gram_send.shape[0]]
    gram_send[...] = gram

    def gram_copy(source, at):
        return pltpu.make_async_remote_copy(
            src_ref=gram_send,
            dst_ref=gram_recv.at[source],
            send_sem=gram_ssem.at[0],
            recv_sem=gram_rsem.at[0],
            device_id={"cols": at},
            device_id_type=MESH,
        )


    @pl.when(col < cols - 1)
    def _():
        pl.semaphore_wait(ready_sem, cols - 1 - col)

    for j in range(1, cols):
        gram_copy(col, (col + j) % cols).start()
    gram_recv[col] = gram
    for t in range(tables):
        pooled_ref[:, t, :] = total_ref[t]
    block = gram_recv.at[pl.ds(0, cols - 1)]
    pltpu.make_async_remote_copy(
        src_ref=block,
        dst_ref=block,
        send_sem=gram_ssem.at[0],
        recv_sem=gram_rsem.at[0],
        device_id={"rows": mate},
        device_id_type=MESH,
    ).wait_recv()
    summed = gram_recv[0]
    for c in range(1, cols):
        summed = summed + gram_recv[c]
    inter_ref[...] = (summed * (width * cols) ** (-0.5))[0:pair]

    def sent(ref, sem):
        pltpu.make_async_remote_copy(
            src_ref=ref,
            dst_ref=ref,
            send_sem=sem,
            recv_sem=gram_rsem.at[0],
            device_id={"rows": mate},
            device_id_type=MESH,
        ).wait_send()

    sent(data_recv.at[pl.ds(0, (n - 1) * tables)], data_ssem.at[0])
    sent(gram_recv.at[pl.ds(0, cols - 1)], gram_ssem.at[0])

    far_sent = fan * (n - 4)
    hub_sent = far_sent + (far_sent + 2 * (fan - 1) if fan > 1 else n - 1)

    def ids_sent(when, tiles):
        @pl.when(when)
        def _():
            sent(ids.at[pl.ds(0, tiles)], id_ssem.at[0])

    ids_sent(jnp.logical_and(leads, hi == 0), fan + n - 2)
    ids_sent(jnp.logical_and(leads, hi == 1), hub_sent)
    ids_sent(jnp.logical_and(leads, hi >= 2), fan * (n - 1))
    if fan > 1:
        ids_sent(jnp.logical_and(col == early, hi == 1), 3 * fan)


def store(pooled_ref, inter_ref, pooled_hbm, inter_hbm, sem):
    copies = [
        pltpu.make_async_copy(pooled_ref, pooled_hbm, sem.at[0]),
        pltpu.make_async_copy(inter_ref, inter_hbm, sem.at[1]),
    ]
    for copy in copies:
        copy.start()
    for copy in copies:
        copy.wait()


def write_out(pooled, inter):
    vmem = pl.BlockSpec(memory_space=pltpu.VMEM)
    hbm = pl.BlockSpec(memory_space=pl.ANY)
    pooled, inter = pl.pallas_call(
        store,
        out_shape=(
            jax.ShapeDtypeStruct(pooled.shape, pooled.dtype),
            jax.ShapeDtypeStruct(inter.shape, inter.dtype),
        ),
        in_specs=[vmem, vmem],
        out_specs=(hbm, hbm),
        scratch_shapes=[pltpu.SemaphoreType.DMA((2,))],
    )(*(pltpu.with_memory_space_constraint(x, pltpu.VMEM) for x in (pooled, inter)))
    return pooled, inter.T


def body(n, cols, tables, dense_features, slot_rows, slot_examples, slot_counts):
    count, range_rows, width = tables.shape
    here = dense_features.shape[0]
    cap = slot_rows.shape[3]
    far = n // 2
    fan = 2 if cols % 2 == 0 else 1
    pairs = (count + 1) * count // 2
    vmem = pl.BlockSpec(memory_space=pltpu.VMEM)
    block = (far, count, here, width)
    chunks = CHUNKS
    any_space = pl.BlockSpec(memory_space=pl.ANY)
    pair_rows = -(-pairs // 8) * 8
    tile = (count, 2 * cap)
    pooled, inter = pl.pallas_call(
        functools.partial(kernel, n, cols, fan),
        out_shape=(
            pltpu.VMEM((here, count, width), jnp.float32),
            pltpu.VMEM((pairs, here), jnp.float32),
        ),
        in_specs=[any_space] * 5,
        out_specs=(vmem, vmem),
        scratch_shapes=[
            pltpu.VMEM((here, width), jnp.float32),
            pltpu.VMEM((2,) + slot_rows.shape, jnp.int32),
            pltpu.SMEM((1, count, n), jnp.int32),
            pltpu.VMEM((count, range_rows, width), jnp.float32),
            pltpu.VMEM((count, range_rows, 2 * width), jnp.bfloat16),
            pltpu.VMEM((4 * n,) + tile, jnp.int32),
            pltpu.VMEM(block, jnp.float32),
            pltpu.VMEM(block, jnp.float32),
            pltpu.VMEM(block, jnp.float32),
            pltpu.VMEM(block, jnp.float32),
            pltpu.VMEM((n * count,) + block[2:], jnp.float32),
            pltpu.VMEM(block[1:], jnp.float32),
            pltpu.VMEM((cols, pair_rows, here), jnp.float32),
            pltpu.VMEM((pair_rows, here), jnp.float32),
            pltpu.SemaphoreType.DMA((4,)),
            pltpu.SemaphoreType.DMA((1,)),
            pltpu.SemaphoreType.DMA((far,)),
            pltpu.SemaphoreType.DMA((1,)),
            pltpu.SemaphoreType.DMA((far - 1, chunks)),
            pltpu.SemaphoreType.DMA((1,)),
            pltpu.SemaphoreType.DMA((far,)),
            pltpu.SemaphoreType.DMA((1,)),
            pltpu.SemaphoreType.DMA((1,)),
            pltpu.SemaphoreType.REGULAR,
        ],
        compiler_params=pltpu.CompilerParams(collective_id=0, has_side_effects=True),
    )(tables, dense_features, slot_rows, slot_examples, slot_counts.transpose(0, 2, 1))
    return write_out(pooled, inter)


def solution(mesh):
    placed = (
        P(None, "rows", "cols"),
        P("rows", "cols"),
        P("rows", None, None, None),
        P("rows", None, None, None),
        P("rows", None, None),
    )
    return jax.shard_map(
        functools.partial(body, mesh.shape["rows"], mesh.shape["cols"]),
        mesh=mesh,
        in_specs=placed,
        out_specs=(P("rows", None, "cols"), P("rows", None)),
        check_vma=False,
    )
```

```python
import functools

import jax
import jax.numpy as jnp
from jax import lax
from jax.experimental import pallas as pl
from jax.experimental.pallas import tpu as pltpu
from jax.sharding import PartitionSpec as P

MESH = pl.DeviceIdType.MESH
CHUNKS = 4
BLOCKS = 2
DEAD = -65536
OWN, DIRECT, PAIR, FORWARD = range(4)
PLANS = {
    4: (
        ((OWN, 0), (PAIR, 2), (PAIR, 3), (DIRECT, 1), (FORWARD, 2), (FORWARD, 3)),
        ((DIRECT, 0), (PAIR, 2), (PAIR, 3), (OWN, 1), (FORWARD, 2), (FORWARD, 3)),
        ((OWN, 2), (PAIR, 0), (PAIR, 1), (DIRECT, 3), (FORWARD, 0), (FORWARD, 1)),
        ((OWN, 3), (DIRECT, 0), (PAIR, 1), (DIRECT, 2), (FORWARD, 1)),
    )
}
ARRIVALS = {4: ((1, 2, 3), (0, 2, 3), (3, 0, 1), (2, 0, 1))}


def repeat(first, last, step, body):
    if (last - first) // step <= 16:
        for k in range(first, last, step):
            body(k)
    else:
        pl.loop(first, last, step=step)(body)


def kernel(
    n,
    cols,
    fan,
    tables_hbm,
    dense_hbm,
    rows_hbm,
    examples_hbm,
    counts_hbm,
    pooled_ref,
    inter_ref,
    dense_ref,
    slots_ref,
    counts_ref,
    table_buf,
    split_buf,
    ids,
    keep,
    cross,
    pair_recv,
    far_send,
    data_recv,
    total_ref,
    gram_recv,
    gram_send,
    load_sem,
    id_ssem,
    id_rsem,
    relay_rsem,
    pair_rsem,
    data_ssem,
    data_rsem,
    gram_ssem,
    gram_rsem,
    ready_sem,
):
    tables, range_rows, width = table_buf.shape
    here = dense_ref.shape[0]
    cap = slots_ref.shape[4]
    far = n // 2
    chunks = pair_rsem.shape[1]
    step = tables // chunks
    me = lax.axis_index("rows")
    col = lax.axis_index("cols")
    hi, lo = me // 2, me % 2
    mate = hi * 2 + (1 - lo)
    near = hi + 1 - 2 * (hi % 2)
    lead = col // fan * fan + fan - 1
    leads = col == lead
    id_send, id_recv, id_relay = ids.at[pl.ds(0, n)], ids.at[pl.ds(n, n)], ids.at[pl.ds(2 * n, max(n - 4, 1))]
    early = lead - fan + 1

    loads = [
        pltpu.make_async_copy(source, target, load_sem.at[i])
        for source, target, i in (
            (counts_hbm, counts_ref, 0),
            (rows_hbm, slots_ref.at[0], 1),
            (examples_hbm, slots_ref.at[1], 1),
            (tables_hbm, table_buf, 2),
            (dense_hbm, dense_ref, 3),
        )
    ]

    barrier = pltpu.get_barrier_semaphore()

    def greet(row, at):
        pl.semaphore_signal(barrier, inc=1, device_id={"rows": row, "cols": at}, device_id_type=MESH)

    @pl.when(hi == 0)
    def _():
        greet(2, early)
        greet(3, early)
        greet(mate, lead)
        repeat(4, n, 1, lambda row: greet(row, lead))

    @pl.when(hi >= 1)
    def _():
        repeat(1, n - 2, 1, lambda j: greet(2 + (me - 2 + j) % (n - 2), lead))

    @pl.when(jnp.logical_and(hi == 1, leads))
    def _():
        greet(0, col)
        greet(1, col)
        for f in range(1, fan):
            greet(mate, lead - f)

    greet(mate, col)
    for c in range(1, cols):
        pl.when(col < c)(functools.partial(greet, me, c))

    for load in loads:
        load.start()

    slot = lax.broadcasted_iota(jnp.int32, (tables, cap), 1)
    half = lax.broadcasted_iota(jnp.int32, (tables, 2 * cap), 1) // cap
    table_id = lax.broadcasted_iota(jnp.int32, (tables, cap), 0)
    loads[0].wait()
    pltpu.make_async_copy(slots_ref, slots_ref, load_sem.at[1]).wait()

    def pack(ref, q, p):
        count = jnp.full((tables, cap), counts_ref[0, 0, p], jnp.int32)
        for t in range(1, tables):
            count = jnp.where(table_id == t, counts_ref[0, t, p], count)
        rows_p = slots_ref[0, 0, p]
        ex_p = jnp.where(slot < count, slots_ref[1, 0, p], DEAD)
        rows_p = jnp.concatenate([rows_p, rows_p], axis=1)
        ref[q] = jnp.where(half == lo, rows_p, jnp.concatenate([ex_p, ex_p], axis=1))

    @pl.when(leads)
    def _():
        repeat(0, n, 1, lambda p: pack(id_send, p, p))

    if fan > 1:

        @pl.when(jnp.logical_and(jnp.logical_not(leads), hi == 1))
        def _():
            for row in (mate, 0, 1):
                pack(id_send, row, row)

    pack(id_recv, me, me)

    loads[3].wait()
    for t in range(tables):
        whole = table_buf[t]
        high = whole.astype(jnp.bfloat16)
        split_buf[t, :, 0:width] = high
        split_buf[t, :, width : 2 * width] = (whole - high.astype(jnp.float32)).astype(jnp.bfloat16)

    first_half = half == 0
    offset = jnp.where(first_half, lo * here, (1 - lo) * here)
    row_iota = lax.broadcasted_iota(jnp.int32, (range_rows, 2 * cap), 0)
    ex_iota = lax.broadcasted_iota(jnp.int32, (2 * here, 2 * cap), 0)

    greeted_lead = col + 1 + fan * (n - 1)
    greeted_lead = jnp.where(hi == 0, col + fan + 3, greeted_lead)
    greeted_lead = jnp.where(hi == 1, col + 1 + fan * (n - 3) + (2 if fan == 1 else 0), greeted_lead)
    greeted_rest = jnp.where(hi == 1, col + 2 + 2 * fan, col + 1)
    pl.semaphore_wait(barrier, jnp.where(leads, greeted_lead, greeted_rest))

    def answer(at):
        pl.semaphore_signal(ready_sem, inc=1, device_id={"cols": at}, device_id_type=MESH)

    def id_copy(src, source, row, at):
        return pltpu.make_async_remote_copy(
            src_ref=src,
            dst_ref=id_recv.at[source],
            send_sem=id_ssem.at[0],
            recv_sem=id_rsem.at[source // 2],
            device_id={"rows": row, "cols": at},
            device_id_type=MESH,
        )

    def ids_wait(first, tiles):
        block = id_recv.at[pl.ds(first, tiles)]
        pltpu.make_async_remote_copy(
            src_ref=block,
            dst_ref=block,
            send_sem=id_ssem.at[0],
            recv_sem=id_rsem.at[first // 2],
            device_id={"rows": mate},
            device_id_type=MESH,
        ).wait_recv()

    def relay_copy():
        block = pl.ds(4, n - 4)
        return pltpu.make_async_remote_copy(
            src_ref=id_send.at[block],
            dst_ref=id_relay,
            send_sem=id_ssem.at[0],
            recv_sem=relay_rsem.at[0],
            device_id={"rows": 2 + lo, "cols": lead},
            device_id_type=MESH,
        )

    def ids_to(row):
        for f in reversed(range(fan)):
            id_copy(id_send.at[row], me, row, lead - f).start()

    def far_ids(first):
        def to(j):
            g = j // 2
            ids_to(jnp.where(g >= hi, g + 1, g) * 2 + (lo + j) % 2)

        repeat(first, n - 2, 1, to)

    @pl.when(jnp.logical_and(leads, hi == 0))
    def _():
        if n > 4:
            relay_copy().start()
        for row in (2, 3):
            id_copy(id_send.at[row], me, row, lead).start()
        ids_to(mate)

    @pl.when(jnp.logical_and(col == early, hi == 1))
    def _():
        for row in (mate, 0, 1):
            ids_to(row)

    @pl.when(jnp.logical_and(leads, hi == 1))
    def _():
        if n > 4:
            relay_copy().wait_recv()

            def relay(j):
                row = n + 3 - j
                for f in reversed(range(fan)):
                    id_copy(id_relay.at[row - 4], lo, row, lead - f).start()

            repeat(4, n, 1, relay)
        far_ids(2)
        ids_wait(0, 2)
        for f in range(1, fan):
            for source in (0, 1):
                id_copy(id_recv.at[source], source, me, lead - f).start()

    @pl.when(jnp.logical_and(leads, hi >= 2))
    def _():
        ids_to(mate)
        far_ids(0)

    for c in range(cols - 1):
        pl.when(col > c)(functools.partial(answer, c))

    def send_block(buf, g, piece, row):
        return pltpu.make_async_remote_copy(
            src_ref=buf.at[g, piece],
            dst_ref=data_recv.at[pl.ds(me * tables + piece.start, piece.size)],
            send_sem=data_ssem.at[0],
            recv_sem=data_rsem.at[hi],
            device_id={"rows": row},
            device_id_type=MESH,
        )

    def slot_of(row):
        return pl.ds(row * tables, tables)

    def data_wait(g, first, blocks):
        block = data_recv.at[pl.ds(first, blocks)]
        pltpu.make_async_remote_copy(
            src_ref=block,
            dst_ref=block,
            send_sem=data_ssem.at[0],
            recv_sem=data_rsem.at[g],
            device_id={"rows": mate},
            device_id_type=MESH,
        ).wait_recv()

    def pair_copy(g, c):
        piece = pl.ds(c * step, step)
        return pltpu.make_async_remote_copy(
            src_ref=cross.at[g, piece],
            dst_ref=pair_recv.at[g, piece],
            send_sem=data_ssem.at[0],
            recv_sem=pair_rsem.at[g % pair_rsem.shape[0], c],
            device_id={"rows": mate},
            device_id_type=MESH,
        )

    def compute(g, then):
        even = id_recv[g * 2]
        odd = id_recv[g * 2 + 1]
        row_of = jnp.where(first_half, even, odd)
        code = jnp.where(first_half, odd, even)
        code = jnp.concatenate([code[:, cap:], code[:, :cap]], axis=1) + offset
        def count(t):
            row_hot = jnp.where(row_iota == row_of[t : t + 1], 1.0, 0.0).astype(jnp.bfloat16)
            ex_hot = jnp.where(ex_iota == code[t : t + 1], 1.0, 0.0).astype(jnp.bfloat16)
            return lax.dot_general(
                ex_hot, row_hot, (((1,), (1,)), ((), ())), preferred_element_type=jnp.float32
            ).astype(jnp.bfloat16)

        def look_up(t, hits):
            both = jnp.dot(hits, split_buf[t], preferred_element_type=jnp.float32)
            return both[:, 0:width] + both[:, width : 2 * width]

        hits = [count(t) for t in range(tables)]
        parts = [look_up(t, hits[t]) for t in range(tables)]
        for t in range(tables):
            keep[g, t] = parts[t][0:here]
            cross[g, t] = parts[t][here : 2 * here]
            if (t + 1) % step == 0:
                then(g, t // step)

    span = tables // BLOCKS

    def pieces(c):
        last = (c + 1) * step
        return [pl.ds(last - span, span)] if last % span == 0 else []

    def direct(g, c):
        for piece in pieces(c):
            send_block(keep, g, piece, g * 2 + lo).start()
            send_block(cross, g, piece, g * 2 + 1 - lo).start()

    def own(g, c):
        for piece in pieces(c):
            send_block(cross, g, piece, mate).start()

    def paired(g, c):
        pair_copy(g, c).start()

    def forward(g):
        for c in range(chunks):
            pair_copy(g, c).wait_recv()
            piece = pl.ds(c * step, step)
            far_send[g, piece] = keep[g, piece] + pair_recv[g, piece]
            send_block(far_send, g, piece, g * 2 + lo).start()

    def ids_of(g, hub=False):
        if hub:
            pl.when(jnp.logical_not(leads))(lambda: ids_wait(g * 2, 2))
        else:
            ids_wait(g * 2, 2)

    def own_group(g):
        ids_wait(mate, 1)
        compute(g, own)

    def add_own(g):
        data_wait(g, mate * tables, tables)
        total_ref[...] = keep[g] + data_recv[slot_of(mate)]

    def add_direct(g):
        data_wait(g, 2 * g * tables, 2 * tables)
        total_ref[...] += data_recv[slot_of(2 * g)] + data_recv[slot_of(2 * g + 1)]

    def add_paired(g):
        data_wait(g, (2 * g + lo) * tables, tables)
        total_ref[...] += data_recv[slot_of(2 * g + lo)]

    def planned(r):
        sends = {DIRECT: direct, PAIR: paired}
        adds = {DIRECT: add_direct, PAIR: add_paired}
        for op, g in PLANS[far][r]:
            if op == OWN:
                own_group(r)
            elif op == FORWARD:
                forward(g)
            else:
                ids_of(g, r == 1 and g == 0)
                compute(g, sends[op])
        add_own(r)
        for g in ARRIVALS[far][r]:
            adds[DIRECT if (DIRECT, r) in PLANS[far][g] else PAIR](g)

    def others(action):
        def both(m):
            q = (hi // 2 + m) % (far // 2)
            action(q * 2)
            action(q * 2 + 1)

        repeat(1, far // 2, 1, both)

    def general():
        @pl.when(hi != 1)
        def _():
            own_group(hi)
            ids_of(near)
            compute(near, direct)

        @pl.when(hi == 1)
        def _():
            ids_of(0, True)
            compute(0, direct)
            own_group(1)

        def far_group(g):
            ids_of(g)
            compute(g, paired)

        others(far_group)
        others(forward)
        add_own(hi)
        add_direct(near)
        others(add_paired)

    if far in PLANS:
        for r in range(far):
            pl.when(hi == r)(functools.partial(planned, r))
    else:
        general()

    loads[4].wait()
    vectors = [dense_ref[...]] + [total_ref[t] for t in range(tables)]
    lane = lax.broadcasted_iota(jnp.int32, (here, 128), 1)
    gram = jnp.zeros((here, 128), jnp.float32)
    pair = 0
    for i in range(tables + 1):
        for j in range(i + 1, tables + 1):
            inner = jnp.sum(vectors[i] * vectors[j], axis=1, keepdims=True)
            gram = jnp.where(lane == pair, inner, gram)
            pair += 1
    gram = gram.T[0 : gram_send.shape[0]]
    gram_send[...] = gram

    def gram_copy(source, at):
        return pltpu.make_async_remote_copy(
            src_ref=gram_send,
            dst_ref=gram_recv.at[source],
            send_sem=gram_ssem.at[0],
            recv_sem=gram_rsem.at[0],
            device_id={"cols": at},
            device_id_type=MESH,
        )


    @pl.when(col < cols - 1)
    def _():
        pl.semaphore_wait(ready_sem, cols - 1 - col)

    for j in range(1, cols):
        gram_copy(col, (col + j) % cols).start()
    gram_recv[col] = gram
    for t in range(tables):
        pooled_ref[:, t, :] = total_ref[t]
    block = gram_recv.at[pl.ds(0, cols - 1)]
    pltpu.make_async_remote_copy(
        src_ref=block,
        dst_ref=block,
        send_sem=gram_ssem.at[0],
        recv_sem=gram_rsem.at[0],
        device_id={"rows": mate},
        device_id_type=MESH,
    ).wait_recv()
    summed = gram_recv[0]
    for c in range(1, cols):
        summed = summed + gram_recv[c]
    inter_ref[...] = (summed * (width * cols) ** (-0.5))[0:pair]

    def sent(ref, sem):
        pltpu.make_async_remote_copy(
            src_ref=ref,
            dst_ref=ref,
            send_sem=sem,
            recv_sem=gram_rsem.at[0],
            device_id={"rows": mate},
            device_id_type=MESH,
        ).wait_send()

    sent(data_recv.at[pl.ds(0, (n - 1) * tables)], data_ssem.at[0])
    sent(gram_recv.at[pl.ds(0, cols - 1)], gram_ssem.at[0])

    far_sent = fan * (n - 4)
    hub_sent = far_sent + (far_sent + 2 * (fan - 1) if fan > 1 else n - 1)

    def ids_sent(when, tiles):
        @pl.when(when)
        def _():
            sent(ids.at[pl.ds(0, tiles)], id_ssem.at[0])

    ids_sent(jnp.logical_and(leads, hi == 0), fan + n - 2)
    ids_sent(jnp.logical_and(leads, hi == 1), hub_sent)
    ids_sent(jnp.logical_and(leads, hi >= 2), fan * (n - 1))
    if fan > 1:
        ids_sent(jnp.logical_and(col == early, hi == 1), 3 * fan)


def store(pooled_ref, inter_ref, pooled_hbm, inter_hbm, sem):
    copies = [
        pltpu.make_async_copy(pooled_ref, pooled_hbm, sem.at[0]),
        pltpu.make_async_copy(inter_ref, inter_hbm, sem.at[1]),
    ]
    for copy in copies:
        copy.start()
    for copy in copies:
        copy.wait()


def write_out(pooled, inter):
    vmem = pl.BlockSpec(memory_space=pltpu.VMEM)
    hbm = pl.BlockSpec(memory_space=pl.ANY)
    pooled, inter = pl.pallas_call(
        store,
        out_shape=(
            jax.ShapeDtypeStruct(pooled.shape, pooled.dtype),
            jax.ShapeDtypeStruct(inter.shape, inter.dtype),
        ),
        in_specs=[vmem, vmem],
        out_specs=(hbm, hbm),
        scratch_shapes=[pltpu.SemaphoreType.DMA((2,))],
    )(*(pltpu.with_memory_space_constraint(x, pltpu.VMEM) for x in (pooled, inter)))
    return pooled, inter.T


def body(n, cols, tables, dense_features, slot_rows, slot_examples, slot_counts):
    count, range_rows, width = tables.shape
    here = dense_features.shape[0]
    cap = slot_rows.shape[3]
    far = n // 2
    fan = 2 if cols % 2 == 0 else 1
    pairs = (count + 1) * count // 2
    vmem = pl.BlockSpec(memory_space=pltpu.VMEM)
    block = (far, count, here, width)
    chunks = CHUNKS
    any_space = pl.BlockSpec(memory_space=pl.ANY)
    pair_rows = -(-pairs // 8) * 8
    tile = (count, 2 * cap)
    pooled, inter = pl.pallas_call(
        functools.partial(kernel, n, cols, fan),
        out_shape=(
            pltpu.VMEM((here, count, width), jnp.float32),
            pltpu.VMEM((pairs, here), jnp.float32),
        ),
        in_specs=[any_space] * 5,
        out_specs=(vmem, vmem),
        scratch_shapes=[
            pltpu.VMEM((here, width), jnp.float32),
            pltpu.VMEM((2,) + slot_rows.shape, jnp.int32),
            pltpu.SMEM((1, count, n), jnp.int32),
            pltpu.VMEM((count, range_rows, width), jnp.float32),
            pltpu.VMEM((count, range_rows, 2 * width), jnp.bfloat16),
            pltpu.VMEM((4 * n,) + tile, jnp.int32),
            pltpu.VMEM(block, jnp.float32),
            pltpu.VMEM(block, jnp.float32),
            pltpu.VMEM(block, jnp.float32),
            pltpu.VMEM(block, jnp.float32),
            pltpu.VMEM((n * count,) + block[2:], jnp.float32),
            pltpu.VMEM(block[1:], jnp.float32),
            pltpu.VMEM((cols, pair_rows, here), jnp.float32),
            pltpu.VMEM((pair_rows, here), jnp.float32),
            pltpu.SemaphoreType.DMA((4,)),
            pltpu.SemaphoreType.DMA((1,)),
            pltpu.SemaphoreType.DMA((far,)),
            pltpu.SemaphoreType.DMA((1,)),
            pltpu.SemaphoreType.DMA((2 if far in PLANS else far, chunks)),
            pltpu.SemaphoreType.DMA((1,)),
            pltpu.SemaphoreType.DMA((far,)),
            pltpu.SemaphoreType.DMA((1,)),
            pltpu.SemaphoreType.DMA((1,)),
            pltpu.SemaphoreType.REGULAR,
        ],
        compiler_params=pltpu.CompilerParams(collective_id=0, has_side_effects=True),
    )(tables, dense_features, slot_rows, slot_examples, slot_counts.transpose(0, 2, 1))
    return write_out(pooled, inter)


def solution(mesh):
    placed = (
        P(None, "rows", "cols"),
        P("rows", "cols"),
        P("rows", None, None, None),
        P("rows", None, None, None),
        P("rows", None, None),
    )
    return jax.shard_map(
        functools.partial(body, mesh.shape["rows"], mesh.shape["cols"]),
        mesh=mesh,
        in_specs=placed,
        out_specs=(P("rows", None, "cols"), P("rows", None)),
        check_vma=False,
    )
```
